16 devices in a mesh: dp: 2 (over y, z), fsdp: 8 (over x, core).
Axes of the slice: x: 4, y: 2, z: 1, core: 2. Of those that a mesh axis runs over, the one named last changes fastest.
The devices are a block of a 4x4x8 slice.
Arguments:
- hidden: bfloat16 [16384, 512], P(('dp', 'fsdp')), parts along dimension 0
- targets: int32 [16384], P(('dp', 'fsdp')), parts along dimension 0
- weight: bfloat16 [32128, 512], P('fsdp')
Outputs:
- output 1: float32 [2], P('dp'), parts along dimension 0
- output 2: float32 [16384, 512], P(('dp', 'fsdp')), parts along dimension 0
- output 3: float32 [64256, 512], P(('dp', 'fsdp')), parts along dimension 0
There are 2 independent parts. The reference program is written for one: setup_inputs(seed, part) draws one part's arguments, and reference() takes and returns one part's arrays. A program takes and returns all parts, laid end to end along the dimension named above; an argument that names none is the same for every part.
All inputs are finite; a program needn't handle non-finite values.
Results may differ from the reference program's by a relative error of at most 0.001.
Values are sent between devices in bfloat16 or wider.
A program may use at most 768 MiB of HBM per device.

```python
import jax
import jax.numpy as jnp
from jax import lax

TOKENS = 8192
VOCAB = 32128
WIDTH = 512
BLOCKS = 8

BLOCK_ROWS = VOCAB // BLOCKS


def setup_inputs(seed: int = 0, part: int = 0) -> dict:
    base_key = jax.random.key(seed)
    key_hid, key_tgt, key_wgt = jax.random.split(base_key, 3)
    key_hid = jax.random.fold_in(key_hid, part)
    key_tgt = jax.random.fold_in(key_tgt, part)
    hidden = jax.random.normal(key_hid, (TOKENS, WIDTH), jnp.float32).astype(jnp.bfloat16)
    targets = jax.random.randint(key_tgt, (TOKENS,), 0, VOCAB, dtype=jnp.int32)
    weight = (jax.random.normal(key_wgt, (VOCAB, WIDTH), jnp.float32) * WIDTH ** -0.5).astype(jnp.bfloat16)
    return {"hidden": hidden, "targets": targets, "weight": weight}


def reference(hidden, targets, weight):
    w_blocks = weight.reshape(BLOCKS, BLOCK_ROWS, WIDTH)
    blk_starts = jnp.arange(BLOCKS, dtype=jnp.int32) * BLOCK_ROWS
    col_ids = jnp.arange(BLOCK_ROWS, dtype=jnp.int32)

    def block_logits(w_blk, blk_start):
        logits = jnp.dot(hidden, w_blk.T, preferred_element_type=jnp.float32)
        is_target = (targets - blk_start)[:, None] == col_ids[None, :]
        return logits, is_target

    def fwd_step(fwd_state, blk_pair):
        run_max, run_sum, tgt_logit = fwd_state
        logits, is_target = block_logits(blk_pair[0], blk_pair[1])
        new_max = jnp.maximum(run_max, jnp.max(logits, axis=1))
        run_sum = run_sum * jnp.exp(run_max - new_max) + jnp.sum(jnp.exp(logits - new_max[:, None]), axis=1)
        tgt_logit = tgt_logit + jnp.sum(jnp.where(is_target, logits, 0.0), axis=1)
        return (new_max, run_sum, tgt_logit), None

    init_state = (jnp.full((TOKENS,), -jnp.inf, jnp.float32), jnp.zeros((TOKENS,), jnp.float32), jnp.zeros((TOKENS,), jnp.float32))
    run_max, run_sum, tgt_logit = lax.scan(fwd_step, init_state, (w_blocks, blk_starts))[0]
    log_norm = run_max + jnp.log(run_sum)
    loss_val = (jnp.sum(log_norm - tgt_logit) / TOKENS).reshape(1)

    def bwd_step(dh_acc, blk_pair):
        logits, is_target = block_logits(blk_pair[0], blk_pair[1])
        dlogits = ((jnp.exp(logits - log_norm[:, None]) - is_target.astype(jnp.float32)) / TOKENS).astype(jnp.bfloat16)
        dh_acc = dh_acc + jnp.dot(dlogits, blk_pair[0], preferred_element_type=jnp.float32)
        dw_blk = jnp.dot(dlogits.T, hidden, preferred_element_type=jnp.float32)
        return dh_acc, dw_blk

    grad_hidden, dw_blocks = lax.scan(bwd_step, jnp.zeros((TOKENS, WIDTH), jnp.float32), (w_blocks, blk_starts))
    return loss_val, grad_hidden, dw_blocks.reshape(VOCAB, WIDTH)
```

```python
import functools

import jax
import jax.numpy as jnp
from jax import lax
from jax.experimental import pallas as pl
from jax.experimental.pallas import tpu as pltpu
from jax.sharding import PartitionSpec as P

F32 = jnp.float32
BF16 = jnp.bfloat16
TOK_TILE = 512
ROW_CHUNK = 1008


def row_chunks(rows):
    return [(start, min(ROW_CHUNK, rows - start)) for start in range(0, rows, ROW_CHUNK)]


def fwd_kernel(w_ref, h_ref, max_ref, sum_ref, z_ref):
    rows = w_ref.shape[0]
    toks = h_ref.shape[0]
    run_max = jnp.full((8, toks), -jnp.inf, F32)
    run_sum = jnp.zeros((8, toks), F32)
    for idx, (start, size) in enumerate(row_chunks(rows)):
        z_new = lax.dot_general(w_ref[start:start + size, :], h_ref[...], (((1,), (1,)), ((), ())), preferred_element_type=F32)
        z_ref[start:start + size, :] = z_new
        z_grp = z_ref[start:start + size, :].reshape(size // 8, 8, toks)
        new_max = jnp.maximum(run_max, jnp.max(z_grp, axis=0))
        run_sum = run_sum * jnp.exp(run_max - new_max) + jnp.sum(jnp.exp(z_grp - new_max[None]), axis=0)
        run_max = new_max
    tot_max = jnp.max(run_max, axis=0, keepdims=True)
    max_ref[...] = tot_max
    sum_ref[...] = jnp.sum(run_sum * jnp.exp(run_max - tot_max), axis=0, keepdims=True)


def bwd_kernel(inv_tokens, w_ref, h_ref, shift_ref, tgt_ref, dh_ref, dw_ref, zt_ref, z_ref, dz_ref):
    rows = w_ref.shape[0]
    toks = h_ref.shape[0]

    @pl.when(pl.program_id(0) == 0)
    def _():
        dw_ref[...] = jnp.zeros_like(dw_ref)

    shift = shift_ref[...]
    tgt = tgt_ref[...]
    zt_sum = jnp.zeros((8, toks), F32)
    for idx, (start, size) in enumerate(row_chunks(rows)):
        z_ref[start:start + size, :] = lax.dot_general(w_ref[start:start + size, :], h_ref[...], (((1,), (1,)), ((), ())), preferred_element_type=F32)
        z = z_ref[start:start + size, :]
        mask = (lax.broadcasted_iota(jnp.int32, (size, toks), 0) + start) == tgt
        prob = jnp.exp(z - shift)
        dz = jnp.where(mask, prob - inv_tokens, prob).astype(BF16)
        zt_sum += jnp.sum(jnp.where(mask, z, 0.0).reshape(size // 8, 8, toks), axis=0)
        dz_ref[start:start + size, :] = dz
        dw_ref[start:start + size, :] += jnp.dot(dz_ref[start:start + size, :], h_ref[...], preferred_element_type=F32)
        dh_part = lax.dot_general(dz_ref[start:start + size, :], w_ref[start:start + size, :], (((0,), (0,)), ((), ())), preferred_element_type=F32)
        if idx == 0:
            dh_ref[...] = dh_part
        else:
            dh_ref[...] += dh_part
    zt_ref[...] = jnp.sum(zt_sum, axis=0, keepdims=True)


def solution(mesh):
    groups = mesh.shape["fsdp"]
    tok_spec = P(("dp", "fsdp"), None)

    def local_head(hidden, targets, weight):
        tok_loc, width = hidden.shape
        rows = weight.shape[0]
        tokens = tok_loc * groups
        tiles = tokens // TOK_TILE
        rank = lax.axis_index("fsdp")
        h_all = lax.all_gather(hidden, "fsdp", tiled=True)
        t_all = (lax.all_gather(targets, "fsdp", tiled=True) - rank * rows).reshape(1, tokens)
        whole_w = pl.BlockSpec((rows, width), lambda i: (0, 0))
        h_spec = pl.BlockSpec((TOK_TILE, width), lambda i: (i, 0))
        row_spec = pl.BlockSpec((1, TOK_TILE), lambda i: (0, i))
        row_shape = jax.ShapeDtypeStruct((1, tokens), F32)
        loc_max, loc_sum = pl.pallas_call(
            fwd_kernel,
            grid=(tiles,),
            in_specs=[whole_w, h_spec],
            out_specs=[row_spec, row_spec],
            out_shape=[row_shape, row_shape],
            scratch_shapes=[pltpu.VMEM((rows, TOK_TILE), F32)],
            name="fwd_stats",
        )(weight, h_all)
        all_max = lax.pmax(loc_max, "fsdp")
        all_sum = lax.psum(loc_sum * jnp.exp(loc_max - all_max), "fsdp")
        lse = all_max + jnp.log(all_sum)
        shift = lse + jnp.log(jnp.float32(tokens))
        dh_part, grad_w, zt = pl.pallas_call(
            functools.partial(bwd_kernel, 1.0 / tokens),
            grid=(tiles,),
            in_specs=[whole_w, h_spec, row_spec, row_spec],
            out_specs=[h_spec, whole_w, row_spec],
            out_shape=[jax.ShapeDtypeStruct((tokens, width), F32), jax.ShapeDtypeStruct((rows, width), F32), row_shape],
            scratch_shapes=[pltpu.VMEM((rows, TOK_TILE), F32), pltpu.VMEM((rows, TOK_TILE), BF16)],
            name="bwd_grads",
        )(weight, h_all, shift, t_all)
        grad_h = lax.psum_scatter(dh_part, "fsdp", scatter_dimension=0, tiled=True)
        loss_val = ((jnp.sum(lse) - lax.psum(jnp.sum(zt), "fsdp")) / tokens).reshape(1)
        return loss_val, grad_h, grad_w

    return jax.shard_map(local_head, mesh=mesh, in_specs=(tok_spec, P(("dp", "fsdp")), P("fsdp", None)), out_specs=(P("dp"), tok_spec, tok_spec), check_vma=False)
```

```python
import functools

import jax
import jax.numpy as jnp
from jax import lax
from jax.experimental import pallas as pl
from jax.experimental.pallas import tpu as pltpu
from jax.sharding import PartitionSpec as P

F32 = jnp.float32
BF16 = jnp.bfloat16
MESH = pl.DeviceIdType.MESH
CORES = 2
ROW_CHUNK = 1008

LEFT, RIGHT, ACROSS = 3, 1, 2
PEERS = [(0, 1), (LEFT, 0), (LEFT, 1), (RIGHT, 0), (RIGHT, 1), (ACROSS, 0), (ACROSS, 1)]
PEER_SLOT = {peer: slot for slot, peer in enumerate(PEERS)}

PAIR_DX = [ACROSS, ACROSS, RIGHT, LEFT, RIGHT, LEFT, 0, 0]
PAIR_HALF = [0, 1, 1, 0, 0, 1, 0, 1]
DX_CODE = sum(v << (2 * q) for q, v in enumerate(PAIR_DX))
HALF_CODE = sum(v << (2 * q) for q, v in enumerate(PAIR_HALF))


def row_chunks(rows):
    return [(start, min(ROW_CHUNK, rows - start)) for start in range(0, rows, ROW_CHUNK)]


def head_kernel(groups, tokens, hid_hbm, tgt_hbm, w_hbm, loss_ref, dh_hbm, dw_hbm,
                h_all, t_all, w_ref, z_ref, dz_ref, dw_ref, pbuf, d2d_in, ring_in, fin_in,
                stat_loc, stat_in, lse_acc, zt_acc, zt_row, zt_in,
                load_sem, ag_send, ag_recv, tgt_send, tgt_recv, stat_send, stat_recv,
                d2d_send, d2d_recv, ici_send, ring_recv, fin_recv, zt_send, zt_recv, out_sem):
    chips = groups // CORES
    me = lax.axis_index("fsdp")
    chip = lax.div(me, CORES)
    core = lax.rem(me, CORES)
    rows, width = w_ref.shape
    half_toks = h_all.shape[2]

    def dev(dx, flip):
        return lax.rem(chip + dx, chips) * CORES + lax.rem(core + flip, CORES)

    def seen_from(peer):
        return PEER_SLOT[((chips - peer[0]) % chips, peer[1])]

    load_h = pltpu.make_async_copy(hid_hbm, h_all.at[me], load_sem.at[0])
    load_t = pltpu.make_async_copy(tgt_hbm, t_all.at[me], load_sem.at[1])
    load_w = pltpu.make_async_copy(w_hbm, w_ref, load_sem.at[2])
    load_h.start()
    load_t.start()
    load_w.start()
    barrier = pltpu.get_barrier_semaphore()
    for peer in PEERS:
        pl.semaphore_signal(barrier, inc=1, device_id={"fsdp": dev(*peer)}, device_id_type=MESH)
    dw_ref[...] = jnp.zeros_like(dw_ref)
    lse_acc[...] = jnp.zeros_like(lse_acc)
    zt_acc[...] = jnp.zeros_like(zt_acc)
    load_h.wait()
    load_t.wait()
    pl.semaphore_wait(barrier, len(PEERS))

    def gather_copy(owner, half, to):
        block = dev(*owner)
        as_seen = PEER_SLOT[((owner[0] - to[0]) % chips, (owner[1] + to[1]) % CORES)]
        idx = as_seen * 2 + half
        return pltpu.make_async_remote_copy(
            src_ref=h_all.at[block, half], dst_ref=h_all.at[block, half], send_sem=ag_send.at[idx], recv_sem=ag_recv.at[idx],
            device_id={"fsdp": dev(*to)}, device_id_type=MESH)

    def gather_recv(owner, half):
        block = dev(*owner)
        idx = PEER_SLOT[owner] * 2 + half
        pltpu.make_async_remote_copy(
            src_ref=h_all.at[block, half], dst_ref=h_all.at[block, half], send_sem=ag_send.at[idx], recv_sem=ag_recv.at[idx],
            device_id={"fsdp": me}, device_id_type=MESH).wait_recv()

    own, partner, left, right, across = (0, 0), (0, 1), (LEFT, 0), (RIGHT, 0), (ACROSS, 0)
    for half, to in [(0, right), (1, left), (0, partner), (1, partner), (1, right), (0, left)]:
        gather_copy(own, half, to).start()

    def target_copy(peer):
        slot = seen_from(peer)
        return pltpu.make_async_remote_copy(
            src_ref=t_all.at[me], dst_ref=t_all.at[me], send_sem=tgt_send.at[slot], recv_sem=tgt_recv.at[slot],
            device_id={"fsdp": dev(*peer)}, device_id_type=MESH)

    for peer in PEERS:
        target_copy(peer).start()
    load_w.wait()

    def stat_copy(peer, block, half):
        return pltpu.make_async_remote_copy(
            src_ref=stat_loc.at[block, half], dst_ref=stat_in.at[seen_from(peer), block, half],
            send_sem=stat_send, recv_sem=stat_recv, device_id={"fsdp": dev(*peer)}, device_id_type=MESH)

    def fwd_step(step, carry):
        grp = lax.div(step, 4)
        sub = lax.rem(step, 4)
        flip = lax.div(sub, 2)
        side = lax.rem(sub, 2)
        dx = lax.rem(lax.div(grp + 1, 2), 2) * (LEFT + (RIGHT - LEFT) * side) + lax.div(grp, 3) * ACROSS
        half = side + lax.div(grp, 2) * (1 - lax.div(grp, 3)) * (1 - 2 * side)
        block = dev(dx, flip)

        @pl.when(step == 2)
        def _():
            gather_recv(partner, 0)
            gather_recv(partner, 1)

        @pl.when(step == 4)
        def _():
            gather_recv(left, 0)
            gather_copy(left, 0, right).start()
            gather_copy(left, 0, partner).start()
            gather_recv(right, 1)
            gather_copy(right, 1, left).start()
            gather_copy(right, 1, partner).start()

        @pl.when(step == 6)
        def _():
            gather_recv((LEFT, 1), 0)
            gather_recv((RIGHT, 1), 1)

        @pl.when(step == 8)
        def _():
            gather_recv(left, 1)
            gather_copy(left, 1, partner).start()
            gather_recv(right, 0)
            gather_copy(right, 0, partner).start()

        @pl.when(step == 10)
        def _():
            gather_recv((LEFT, 1), 1)
            gather_recv((RIGHT, 1), 0)

        @pl.when(step == 12)
        def _():
            gather_recv(across, 0)
            gather_copy(across, 0, partner).start()
            gather_recv(across, 1)
            gather_copy(across, 1, partner).start()

        @pl.when(step == 14)
        def _():
            gather_recv((ACROSS, 1), 0)
            gather_recv((ACROSS, 1), 1)

        run_max = jnp.full((8, half_toks), -jnp.inf, F32)
        run_sum = jnp.zeros((8, half_toks), F32)
        for start, size in row_chunks(rows):
            z_ref[start:start + size, :] = lax.dot_general(
                w_ref[start:start + size, :], h_all[block, half], (((1,), (1,)), ((), ())), preferred_element_type=F32)
            z_grp = z_ref[start:start + size, :].reshape(size // 8, 8, half_toks)
            new_max = jnp.maximum(run_max, jnp.max(z_grp, axis=0))
            run_sum = run_sum * jnp.exp(run_max - new_max) + jnp.sum(jnp.exp(z_grp - new_max[None]), axis=0)
            run_max = new_max
        tot_max = jnp.max(run_max, axis=0, keepdims=True)
        stat_loc[block, half, 0] = tot_max
        stat_loc[block, half, 1] = jnp.sum(run_sum * jnp.exp(run_max - tot_max), axis=0, keepdims=True)
        for peer in PEERS:
            stat_copy(peer, block, half).start()
        return carry

    lax.fori_loop(0, 2 * groups, fwd_step, 0)

    for peer in PEERS:
        target_copy(peer).wait_recv()
    all_stats = pltpu.make_async_remote_copy(
        src_ref=stat_in, dst_ref=stat_in, send_sem=stat_send, recv_sem=stat_recv, device_id={"fsdp": me}, device_id_type=MESH)
    all_stats.wait_recv()

    def d2d_copy(pair, slot):
        return pltpu.make_async_remote_copy(
            src_ref=pbuf.at[slot], dst_ref=d2d_in.at[pair], send_sem=d2d_send.at[slot], recv_sem=d2d_recv.at[pair],
            device_id={"fsdp": dev(*partner)}, device_id_type=MESH)

    def ici_copy(pair):
        dx, half = PAIR_DX[pair], PAIR_HALF[pair]
        if dx == ACROSS:
            to = right if half == 0 else left
            dst, recv = ring_in.at[half], ring_recv.at[half]
        else:
            to = (dx, 0)
            from_side = 0 if dx == RIGHT else 1
            dst, recv = fin_in.at[from_side, half], fin_recv.at[from_side * 2 + half]
        return pltpu.make_async_remote_copy(
            src_ref=pbuf.at[2 + pair], dst_ref=dst, send_sem=ici_send.at[pair], recv_sem=recv,
            device_id={"fsdp": dev(*to)}, device_id_type=MESH)

    def add_into(slot, sources):
        def body(i, carry):
            sl = pl.ds(pl.multiple_of(i * 64, 64), 64)
            tot = pbuf[slot, sl, :]
            for src in sources:
                tot = tot + src[sl, :]
            pbuf[slot, sl, :] = tot
            return carry
        lax.fori_loop(0, half_toks // 64, body, 0)

    inv_tokens = 1.0 / tokens
    log_tokens = jnp.log(jnp.float32(tokens))

    def bwd_step(step, carry):
        pair = lax.div(step, 2)
        flip = 1 - lax.rem(step, 2)
        dx = lax.rem(lax.shift_right_logical(jnp.int32(DX_CODE), 2 * pair), 4)
        half = lax.rem(lax.shift_right_logical(jnp.int32(HALF_CODE), 2 * pair), 4)
        block = dev(dx, flip)
        slot = flip * lax.rem(pair, 2) + (1 - flip) * (2 + pair)

        for pair_s in range(2, 8):
            @pl.when(step == 2 * pair_s)
            def _():
                d2d_copy(pair_s - 2, pair_s % 2).wait_send()

        maxes = [stat_loc[block, half, 0]] + [stat_in[i, block, half, 0] for i in range(len(PEERS))]
        sums = [stat_loc[block, half, 1]] + [stat_in[i, block, half, 1] for i in range(len(PEERS))]
        tot_max = functools.reduce(jnp.maximum, maxes)
        tot_sum = sum(s * jnp.exp(m - tot_max) for m, s in zip(maxes, sums))
        lse = tot_max + jnp.log(tot_sum)
        lse_acc[...] += lse
        shift = lse + log_tokens
        tgt = t_all[block, half] - me * rows
        zt_sum = zt_acc[...]
        h_tile = h_all.at[block, half]
        for idx, (start, size) in enumerate(row_chunks(rows)):
            sl = slice(start, start + size)
            z_ref[sl, :] = lax.dot_general(w_ref[sl, :], h_tile[...], (((1,), (1,)), ((), ())), preferred_element_type=F32)
            z = z_ref[sl, :]
            mask = (lax.broadcasted_iota(jnp.int32, (size, half_toks), 0) + start) == tgt
            prob = jnp.exp(z - shift)
            dz_ref[sl, :] = jnp.where(mask, prob - inv_tokens, prob).astype(BF16)
            zt_sum += jnp.sum(jnp.where(mask, z, 0.0).reshape(size // 8, 8, half_toks), axis=0)
            dw_ref[sl, :] += jnp.dot(dz_ref[sl, :], h_tile[...], preferred_element_type=F32)
            dh_part = lax.dot_general(dz_ref[sl, :], w_ref[sl, :], (((0,), (0,)), ((), ())), preferred_element_type=F32)
            if idx == 0:
                pbuf[slot] = dh_part
            else:
                pbuf[slot] += dh_part
        zt_acc[...] = zt_sum

        for pair_s in range(8):
            @pl.when(step == 2 * pair_s)
            def _():
                d2d_copy(pair_s, pair_s % 2).start()

            @pl.when(step == 2 * pair_s + 1)
            def _():
                d2d_copy(pair_s, pair_s % 2).wait_recv()
                sources = [d2d_in.at[pair_s]]
                dx_s, half_s = PAIR_DX[pair_s], PAIR_HALF[pair_s]
                if (dx_s, half_s) == (RIGHT, 0):
                    ici_copy(0).wait_recv()
                    sources.append(ring_in.at[0])
                if (dx_s, half_s) == (LEFT, 1):
                    ici_copy(1).wait_recv()
                    sources.append(ring_in.at[1])
                if dx_s == 0:
                    for pair_r in range(2, 6):
                        if PAIR_HALF[pair_r] == half_s:
                            ici_copy(pair_r).wait_recv()
                            sources.append(fin_in.at[0 if PAIR_DX[pair_r] == RIGHT else 1, half_s])
                add_into(2 + pair_s, sources)
                if dx_s == 0:
                    pltpu.make_async_copy(pbuf.at[2 + pair_s], dh_hbm.at[half_s], out_sem.at[half_s]).start()
                else:
                    ici_copy(pair_s).start()
        return carry

    lax.fori_loop(0, 2 * groups, bwd_step, 0)

    out_w = pltpu.make_async_copy(dw_ref, dw_hbm, out_sem.at[2])
    out_w.start()
    zt_row[...] = jnp.sum(zt_acc[...], axis=0, keepdims=True)

    def zt_copy(peer):
        slot = seen_from(peer)
        return pltpu.make_async_remote_copy(
            src_ref=zt_row, dst_ref=zt_in.at[slot], send_sem=zt_send.at[slot], recv_sem=zt_recv.at[slot],
            device_id={"fsdp": dev(*peer)}, device_id_type=MESH)

    for peer in PEERS:
        zt_copy(peer).start()
    for peer in PEERS:
        zt_copy(peer).wait()
    tot = lse_acc[...] - zt_row[...]
    for i in range(len(PEERS)):
        tot = tot - zt_in[i]
    loss_ref[...] = jnp.broadcast_to(jnp.sum(tot, axis=1, keepdims=True) * inv_tokens, loss_ref.shape)

    for owner, half, to in (
            [(own, h, to) for h in range(2) for to in (right, left, partner)]
            + [(left, 0, right), (right, 1, left)]
            + [(side, h, partner) for side in (left, right, across) for h in range(2)]):
        gather_copy(owner, half, to).wait_send()
    for peer in PEERS:
        target_copy(peer).wait_send()
    all_stats.wait_send()
    d2d_copy(6, 0).wait_send()
    d2d_copy(7, 1).wait_send()
    for pair in range(6):
        ici_copy(pair).wait_send()
    for half in range(2):
        pltpu.make_async_copy(pbuf.at[8 + half], dh_hbm.at[half], out_sem.at[half]).wait()
    out_w.wait()


def solution(mesh):
    groups = mesh.shape["fsdp"]
    tok_spec = P(("dp", "fsdp"), None)

    def local_head(hidden, targets, weight):
        tok_loc, width = hidden.shape
        rows = weight.shape[0]
        tokens = tok_loc * groups
        half = tok_loc // 2
        peers = len(PEERS)
        any_spec = pl.BlockSpec(memory_space=pl.ANY)
        vmem, dma = pltpu.VMEM, pltpu.SemaphoreType.DMA
        loss_row, grad_h, grad_w = pl.pallas_call(
            functools.partial(head_kernel, groups, tokens),
            in_specs=[any_spec] * 3,
            out_specs=[pl.BlockSpec(memory_space=pltpu.VMEM), any_spec, any_spec],
            out_shape=[jax.ShapeDtypeStruct((1, 128), F32), jax.ShapeDtypeStruct((2, half, width), F32), jax.ShapeDtypeStruct((rows, width), F32)],
            scratch_shapes=[
                vmem((groups, 2, half, width), BF16),
                vmem((groups, 2, 1, half), jnp.int32),
                vmem((rows, width), BF16),
                vmem((rows, half), F32),
                vmem((rows, half), BF16),
                vmem((rows, width), F32),
                vmem((10, half, width), F32),
                vmem((8, half, width), F32),
                vmem((2, half, width), F32),
                vmem((2, 2, half, width), F32),
                vmem((groups, 2, 2, 1, half), F32),
                vmem((peers, groups, 2, 2, 1, half), F32),
                vmem((1, half), F32),
                vmem((8, half), F32),
                vmem((1, half), F32),
                vmem((peers, 1, half), F32),
                dma((3,)), dma((2 * peers,)), dma((2 * peers,)), dma((peers,)), dma((peers,)), dma, dma,
                dma((2,)), dma((8,)), dma((6,)), dma((2,)), dma((4,)), dma((peers,)), dma((peers,)), dma((3,)),
            ],
            compiler_params=pltpu.CompilerParams(collective_id=0, has_side_effects=True, vmem_limit_bytes=67_000_000),
            name="head",
        )(hidden.reshape(2, half, width), targets.reshape(2, 1, half), weight)
        return loss_row[0, :1], grad_h.reshape(tok_loc, width), grad_w

    return jax.shard_map(local_head, mesh=mesh, in_specs=(tok_spec, P(("dp", "fsdp")), P("fsdp", None)), out_specs=(P("dp"), tok_spec, tok_spec), check_vma=False)
```

```python
import functools

import jax
import jax.numpy as jnp
from jax import lax
from jax.experimental import pallas as pl
from jax.experimental.pallas import tpu as pltpu
from jax.sharding import PartitionSpec as P

F32 = jnp.float32
BF16 = jnp.bfloat16
MESH = pl.DeviceIdType.MESH
CORES = 2
ROW_CHUNK = 1008

LEFT, RIGHT, ACROSS = 3, 1, 2
PEERS = [(0, 1), (LEFT, 0), (LEFT, 1), (RIGHT, 0), (RIGHT, 1), (ACROSS, 0), (ACROSS, 1)]
PEER_SLOT = {peer: slot for slot, peer in enumerate(PEERS)}

PAIR_DX = [ACROSS, ACROSS, RIGHT, LEFT, RIGHT, LEFT, 0, 0]
PAIR_HALF = [0, 1, 1, 0, 0, 1, 0, 1]
DX_CODE = sum(v << (2 * q) for q, v in enumerate(PAIR_DX))
HALF_CODE = sum(v << (2 * q) for q, v in enumerate(PAIR_HALF))


def row_chunks(rows):
    return [(start, min(ROW_CHUNK, rows - start)) for start in range(0, rows, ROW_CHUNK)]


def head_kernel(groups, tokens, hid_hbm, tgt_hbm, w_hbm, loss_ref, dh_hbm, dw_hbm, z_hbm,
                h_all, t_all, w_ref, z_ref, dz_ref, dw_ref, pbuf, d2d_in, ring_in, fin_in,
                stat_loc, stat_in, lse_acc, zt_acc, zt_row, zt_in,
                load_sem, ag_send, ag_recv, tgt_send, tgt_recv, stat_send, stat_recv,
                d2d_send, d2d_recv, ici_send, ring_recv, fin_recv, zt_send, zt_recv, out_sem, z_out, z_back):
    chips = groups // CORES
    me = lax.axis_index("fsdp")
    chip = lax.div(me, CORES)
    core = lax.rem(me, CORES)
    rows, width = w_ref.shape
    half_toks = h_all.shape[2]

    def dev(dx, flip):
        return lax.rem(chip + dx, chips) * CORES + lax.rem(core + flip, CORES)

    def seen_from(peer):
        return PEER_SLOT[((chips - peer[0]) % chips, peer[1])]

    load_h = pltpu.make_async_copy(hid_hbm, h_all.at[me], load_sem.at[0])
    load_t = pltpu.make_async_copy(tgt_hbm, t_all.at[me], load_sem.at[1])
    load_w = pltpu.make_async_copy(w_hbm, w_ref, load_sem.at[2])
    load_h.start()
    load_t.start()
    load_w.start()
    barrier = pltpu.get_barrier_semaphore()
    for peer in PEERS:
        pl.semaphore_signal(barrier, inc=1, device_id={"fsdp": dev(*peer)}, device_id_type=MESH)
    dw_ref[...] = jnp.zeros_like(dw_ref)
    lse_acc[...] = jnp.zeros_like(lse_acc)
    zt_acc[...] = jnp.zeros_like(zt_acc)

    def z_store(buf, slot, chunk):
        start, size = row_chunks(rows)[chunk]
        return pltpu.make_async_copy(z_ref.at[buf, start:start + size], z_hbm.at[slot, start:start + size], z_out.at[buf, chunk])

    def z_load(buf, slot):
        return pltpu.make_async_copy(z_hbm.at[slot], z_ref.at[buf], z_back.at[buf])

    num_chunks = len(row_chunks(rows))
    for chunk, (start, size) in enumerate(row_chunks(rows)):
        pltpu.make_async_copy(dw_ref.at[start:start + size], z_hbm.at[2 * groups, start:start + size], z_out.at[1, chunk]).start()
    load_h.wait()
    load_t.wait()
    pl.semaphore_wait(barrier, len(PEERS))

    def gather_copy(owner, half, to):
        block = dev(*owner)
        as_seen = PEER_SLOT[((owner[0] - to[0]) % chips, (owner[1] + to[1]) % CORES)]
        idx = as_seen * 2 + half
        return pltpu.make_async_remote_copy(
            src_ref=h_all.at[block, half], dst_ref=h_all.at[block, half], send_sem=ag_send.at[idx], recv_sem=ag_recv.at[idx],
            device_id={"fsdp": dev(*to)}, device_id_type=MESH)

    def gather_recv(owner, half):
        block = dev(*owner)
        idx = PEER_SLOT[owner] * 2 + half
        pltpu.make_async_remote_copy(
            src_ref=h_all.at[block, half], dst_ref=h_all.at[block, half], send_sem=ag_send.at[idx], recv_sem=ag_recv.at[idx],
            device_id={"fsdp": me}, device_id_type=MESH).wait_recv()

    own, partner, left, right, across = (0, 0), (0, 1), (LEFT, 0), (RIGHT, 0), (ACROSS, 0)
    for half, to in [(0, right), (1, left), (0, partner), (1, partner), (1, right), (0, left)]:
        gather_copy(own, half, to).start()

    def target_copy(peer):
        slot = seen_from(peer)
        return pltpu.make_async_remote_copy(
            src_ref=t_all.at[me], dst_ref=t_all.at[me], send_sem=tgt_send.at[slot], recv_sem=tgt_recv.at[slot],
            device_id={"fsdp": dev(*peer)}, device_id_type=MESH)

    for peer in PEERS:
        target_copy(peer).start()
    load_w.wait()

    def stat_copy(peer, block, half):
        return pltpu.make_async_remote_copy(
            src_ref=stat_loc.at[block, half], dst_ref=stat_in.at[seen_from(peer), block, half],
            send_sem=stat_send, recv_sem=stat_recv, device_id={"fsdp": dev(*peer)}, device_id_type=MESH)

    def fwd_half(buf, block, half):
        run_max = jnp.full((8, half_toks), -jnp.inf, F32)
        run_sum = jnp.zeros((8, half_toks), F32)
        for chunk, (start, size) in enumerate(row_chunks(rows)):
            sl = slice(start, start + size)
            z_ref[buf, sl, :] = lax.dot_general(
                w_ref[sl, :], h_all[block, half], (((1,), (1,)), ((), ())), preferred_element_type=F32)
            z_grp = z_ref[buf, sl, :].reshape(size // 8, 8, half_toks)
            new_max = jnp.maximum(run_max, jnp.max(z_grp, axis=0))
            run_sum = run_sum * jnp.exp(run_max - new_max) + jnp.sum(jnp.exp(z_grp - new_max[None]), axis=0)
            run_max = new_max
            z_store(buf, 2 * block + half, chunk).start()
        tot_max = jnp.max(run_max, axis=0, keepdims=True)
        stat_loc[block, half, 0] = tot_max
        stat_loc[block, half, 1] = jnp.sum(run_sum * jnp.exp(run_max - tot_max), axis=0, keepdims=True)
        for peer in PEERS:
            stat_copy(peer, block, half).start()

    def fwd_pair(step, carry):
        grp = lax.div(step, 2)
        flip = lax.rem(step, 2)
        mixed = lax.rem(lax.div(grp + 1, 2), 2)

        @pl.when(step == 1)
        def _():
            gather_recv(partner, 0)
            gather_recv(partner, 1)

        @pl.when(step == 2)
        def _():
            gather_recv(left, 0)
            gather_copy(left, 0, right).start()
            gather_copy(left, 0, partner).start()
            gather_recv(right, 1)
            gather_copy(right, 1, left).start()
            gather_copy(right, 1, partner).start()

        @pl.when(step == 3)
        def _():
            gather_recv((LEFT, 1), 0)
            gather_recv((RIGHT, 1), 1)

        @pl.when(step == 4)
        def _():
            gather_recv(left, 1)
            gather_copy(left, 1, partner).start()
            gather_recv(right, 0)
            gather_copy(right, 0, partner).start()

        @pl.when(step == 5)
        def _():
            gather_recv((LEFT, 1), 1)
            gather_recv((RIGHT, 1), 0)

        @pl.when(step == 6)
        def _():
            gather_recv(across, 0)
            gather_copy(across, 0, partner).start()
            gather_recv(across, 1)
            gather_copy(across, 1, partner).start()

        @pl.when(step == 7)
        def _():
            gather_recv((ACROSS, 1), 0)
            gather_recv((ACROSS, 1), 1)

        @pl.when(step > 0)
        def _():
            for chunk in range(num_chunks):
                z_store(0, 0, chunk).wait()

        for side in range(2):
            dx = mixed * (LEFT + (RIGHT - LEFT) * side) + lax.div(grp, 3) * ACROSS
            half = side + lax.div(grp, 2) * (1 - lax.div(grp, 3)) * (1 - 2 * side)
            if side == 1:
                for chunk in range(num_chunks):
                    z_store(1, 0, chunk).wait()
            fwd_half(side, dev(dx, flip), half)
        return carry

    lax.fori_loop(0, groups, fwd_pair, 0)

    for buf in range(2):
        for chunk in range(num_chunks):
            z_store(buf, 0, chunk).wait()

    for peer in PEERS:
        target_copy(peer).wait_recv()
    all_stats = pltpu.make_async_remote_copy(
        src_ref=stat_in, dst_ref=stat_in, send_sem=stat_send, recv_sem=stat_recv, device_id={"fsdp": me}, device_id_type=MESH)
    all_stats.wait_recv()

    def d2d_copy(slot):
        return pltpu.make_async_remote_copy(
            src_ref=pbuf.at[slot], dst_ref=d2d_in.at[slot], send_sem=d2d_send.at[slot], recv_sem=d2d_recv.at[slot],
            device_id={"fsdp": dev(*partner)}, device_id_type=MESH)

    def ici_copy(pair):
        dx, half = PAIR_DX[pair], PAIR_HALF[pair]
        if dx == ACROSS:
            to = right if half == 0 else left
            dst, recv = ring_in.at[half], ring_recv.at[half]
        else:
            to = (dx, 0)
            from_side = 0 if dx == RIGHT else 1
            dst, recv = fin_in.at[from_side, half], fin_recv.at[from_side * 2 + half]
        return pltpu.make_async_remote_copy(
            src_ref=pbuf.at[2 + pair], dst_ref=dst, send_sem=ici_send.at[pair], recv_sem=recv,
            device_id={"fsdp": dev(*to)}, device_id_type=MESH)

    def add_into(slot, sources):
        def body(i, carry):
            sl = pl.ds(pl.multiple_of(i * 64, 64), 64)
            tot = pbuf[slot, sl, :]
            for src in sources:
                tot = tot + src[sl, :]
            pbuf[slot, sl, :] = tot
            return carry
        lax.fori_loop(0, half_toks // 64, body, 0)

    inv_tokens = 1.0 / tokens
    log_tokens = jnp.log(jnp.float32(tokens))

    def pair_block(pair, flip):
        dx = lax.rem(lax.shift_right_logical(jnp.int32(DX_CODE), 2 * pair), 4)
        half = lax.rem(lax.shift_right_logical(jnp.int32(HALF_CODE), 2 * pair), 4)
        return dev(dx, flip), half

    def z_slot(pair, flip):
        block, half = pair_block(pair, flip)
        return 2 * block + half

    def bwd_half(buf, slot, block, half):
        maxes = [stat_loc[block, half, 0]] + [stat_in[i, block, half, 0] for i in range(len(PEERS))]
        sums = [stat_loc[block, half, 1]] + [stat_in[i, block, half, 1] for i in range(len(PEERS))]
        tot_max = functools.reduce(jnp.maximum, maxes)
        tot_sum = sum(s * jnp.exp(m - tot_max) for m, s in zip(maxes, sums))
        lse = tot_max + jnp.log(tot_sum)
        lse_acc[...] += lse
        shift = lse + log_tokens
        tgt = t_all[block, half] - me * rows
        zt_sum = zt_acc[...]
        h_tile = h_all.at[block, half]
        for idx, (start, size) in enumerate(row_chunks(rows)):
            sl = slice(start, start + size)
            z = z_ref[buf, sl, :]
            mask = (lax.broadcasted_iota(jnp.int32, (size, half_toks), 0) + start) == tgt
            prob = jnp.exp(z - shift)
            dz_ref[sl, :] = jnp.where(mask, prob - inv_tokens, prob).astype(BF16)
            zt_sum += jnp.sum(jnp.where(mask, z, 0.0).reshape(size // 8, 8, half_toks), axis=0)
            dw_ref[sl, :] += jnp.dot(dz_ref[sl, :], h_tile[...], preferred_element_type=F32)
            dh_part = lax.dot_general(dz_ref[sl, :], w_ref[sl, :], (((0,), (0,)), ((), ())), preferred_element_type=F32)
            if idx == 0:
                pbuf[slot] = dh_part
            else:
                pbuf[slot] += dh_part
        zt_acc[...] = zt_sum

    def bwd_pair(pair, carry):
        odd = lax.rem(pair, 2)

        @pl.when(pair >= 2)
        def _():
            d2d_copy(odd).wait_send()

        @pl.when(pair >= 1)
        def _():
            z_load(0, 0).wait()

        block, half = pair_block(pair, 1)
        bwd_half(0, odd, block, half)
        d2d_copy(odd).start()
        z_load(0, z_slot(lax.rem(pair + 1, groups), 1)).start()
        z_load(1, 0).wait()
        block, half = pair_block(pair, 0)
        bwd_half(1, 2 + pair, block, half)

        @pl.when(pair < groups - 1)
        def _():
            z_load(1, z_slot(pair + 1, 0)).start()

        d2d_copy(odd).wait_recv()
        for pair_s in range(8):
            @pl.when(pair == pair_s)
            def _():
                sources = [d2d_in.at[pair_s % 2]]
                dx_s, half_s = PAIR_DX[pair_s], PAIR_HALF[pair_s]
                if (dx_s, half_s) == (RIGHT, 0):
                    ici_copy(0).wait_recv()
                    sources.append(ring_in.at[0])
                if (dx_s, half_s) == (LEFT, 1):
                    ici_copy(1).wait_recv()
                    sources.append(ring_in.at[1])
                if dx_s == 0:
                    for pair_r in range(2, 6):
                        if PAIR_HALF[pair_r] == half_s:
                            ici_copy(pair_r).wait_recv()
                            sources.append(fin_in.at[0 if PAIR_DX[pair_r] == RIGHT else 1, half_s])
                add_into(2 + pair_s, sources)
                if dx_s == 0:
                    pltpu.make_async_copy(pbuf.at[2 + pair_s], dh_hbm.at[half_s], out_sem.at[half_s]).start()
                else:
                    ici_copy(pair_s).start()
        return carry

    z_load(1, z_slot(0, 0)).start()
    lax.fori_loop(0, groups, bwd_pair, 0)

    out_w = pltpu.make_async_copy(dw_ref, dw_hbm, out_sem.at[2])
    out_w.start()
    zt_row[...] = jnp.sum(zt_acc[...], axis=0, keepdims=True)

    def zt_copy(peer):
        slot = seen_from(peer)
        return pltpu.make_async_remote_copy(
            src_ref=zt_row, dst_ref=zt_in.at[slot], send_sem=zt_send.at[slot], recv_sem=zt_recv.at[slot],
            device_id={"fsdp": dev(*peer)}, device_id_type=MESH)

    for peer in PEERS:
        zt_copy(peer).start()
    for peer in PEERS:
        zt_copy(peer).wait()
    tot = lse_acc[...] - zt_row[...]
    for i in range(len(PEERS)):
        tot = tot - zt_in[i]
    loss_ref[...] = jnp.broadcast_to(jnp.sum(tot, axis=1, keepdims=True) * inv_tokens, loss_ref.shape)

    for owner, half, to in (
            [(own, h, to) for h in range(2) for to in (right, left, partner)]
            + [(left, 0, right), (right, 1, left)]
            + [(side, h, partner) for side in (left, right, across) for h in range(2)]):
        gather_copy(owner, half, to).wait_send()
    for peer in PEERS:
        target_copy(peer).wait_send()
    all_stats.wait_send()
    d2d_copy(0).wait_send()
    d2d_copy(1).wait_send()
    z_load(0, 0).wait()
    for pair in range(6):
        ici_copy(pair).wait_send()
    for half in range(2):
        pltpu.make_async_copy(pbuf.at[8 + half], dh_hbm.at[half], out_sem.at[half]).wait()
    out_w.wait()


def solution(mesh):
    groups = mesh.shape["fsdp"]
    tok_spec = P(("dp", "fsdp"), None)

    def local_head(hidden, targets, weight):
        tok_loc, width = hidden.shape
        rows = weight.shape[0]
        tokens = tok_loc * groups
        half = tok_loc // 2
        peers = len(PEERS)
        any_spec = pl.BlockSpec(memory_space=pl.ANY)
        vmem, dma = pltpu.VMEM, pltpu.SemaphoreType.DMA
        loss_row, grad_h, grad_w, _ = pl.pallas_call(
            functools.partial(head_kernel, groups, tokens),
            in_specs=[any_spec] * 3,
            out_specs=[pl.BlockSpec(memory_space=pltpu.VMEM), any_spec, any_spec, any_spec],
            out_shape=[jax.ShapeDtypeStruct((1, 128), F32), jax.ShapeDtypeStruct((2, half, width), F32), jax.ShapeDtypeStruct((rows, width), F32), jax.ShapeDtypeStruct((2 * groups + 1, rows, half), F32)],
            scratch_shapes=[
                vmem((groups, 2, half, width), BF16),
                vmem((groups, 2, 1, half), jnp.int32),
                vmem((rows, width), BF16),
                vmem((2, rows, half), F32),
                vmem((rows, half), BF16),
                vmem((rows, width), F32),
                vmem((10, half, width), F32),
                vmem((2, half, width), F32),
                vmem((2, half, width), F32),
                vmem((2, 2, half, width), F32),
                vmem((groups, 2, 2, 1, half), F32),
                vmem((peers, groups, 2, 2, 1, half), F32),
                vmem((1, half), F32),
                vmem((8, half), F32),
                vmem((1, half), F32),
                vmem((peers, 1, half), F32),
                dma((3,)), dma((2 * peers,)), dma((2 * peers,)), dma((peers,)), dma((peers,)), dma, dma,
                dma((2,)), dma((2,)), dma((6,)), dma((2,)), dma((4,)), dma((peers,)), dma((peers,)), dma((3,)),
                dma((2, len(row_chunks(rows)))), dma((2,)),
            ],
            compiler_params=pltpu.CompilerParams(collective_id=0, has_side_effects=True, vmem_limit_bytes=67_000_000),
            name="head",
        )(hidden.reshape(2, half, width), targets.reshape(2, 1, half), weight)
        return loss_row[0, :1], grad_h.reshape(tok_loc, width), grad_w

    return jax.shard_map(local_head, mesh=mesh, in_specs=(tok_spec, P(("dp", "fsdp")), P("fsdp", None)), out_specs=(P("dp"), tok_spec, tok_spec), check_vma=False)
```

```python
import functools

import jax
import jax.numpy as jnp
from jax import lax
from jax.experimental import pallas as pl
from jax.experimental.pallas import tpu as pltpu
from jax.sharding import PartitionSpec as P

F32 = jnp.float32
BF16 = jnp.bfloat16
MESH = pl.DeviceIdType.MESH
CORES = 2
FWD_CHUNK = 512
BWD_CHUNK = 1008
TAIL_ROWS = 512

LEFT, RIGHT, ACROSS = 3, 1, 2
OWN, PARTNER = (0, 0), (0, 1)
PEERS = [PARTNER, (LEFT, 0), (LEFT, 1), (RIGHT, 0), (RIGHT, 1), (ACROSS, 0), (ACROSS, 1)]
PEER_SLOT = {peer: slot for slot, peer in enumerate(PEERS)}

def tile_id(kind, flip, j):
    if kind == "mixed":
        return 4 + 2 * flip + 4 * (j // 2) + j % 2
    return {"own": 0, "across": 12}[kind] + 2 * flip + j


def place(owner, quarter):
    dx, flip = owner
    if dx in (LEFT, RIGHT):
        return tile_id("mixed", flip, quarter), 0 if dx == RIGHT else 1
    return tile_id("own" if dx == 0 else "across", flip, quarter // 2), quarter % 2


PAIRS = [("across", 0), ("across", 1)] + [("mixed", j) for j in range(4)] + [("own", 0), ("own", 1)]
PAIR_CODE = sum(tile_id(kind, 0, j) << (4 * q) for q, (kind, j) in enumerate(PAIRS))


def chunks(rows, step):
    return [(start, min(step, rows - start)) for start in range(0, rows, step)]


def head_kernel(groups, tokens, hid_hbm, tgt_hbm, w_hbm, loss_ref, dh_hbm, dw_hbm, dz_hbm, htail_hbm, z_hbm,
                h_all, t_all, w_ref, z_ref, dz_ref, dw_ref, pbuf, d2d_in, ring_in, fin_in,
                stat_loc, stat_in, lse_acc, zt_acc, zt_row, zt_in,
                load_sem, ag_send, ag_recv, tgt_send, tgt_recv, stat_send, stat_recv,
                d2d_send, d2d_recv, ici_send, ring_recv, fin_recv, zt_send, zt_recv, out_sem, z_out, z_back):
    chips = groups // CORES
    me = lax.axis_index("fsdp")
    chip = lax.div(me, CORES)
    core = lax.rem(me, CORES)
    rows, width = w_ref.shape
    tile = h_all.shape[1]
    quarter_toks = tile // 2
    parts = [pl.ds(0, quarter_toks), pl.ds(quarter_toks, quarter_toks)]
    left, right, across = (LEFT, 0), (RIGHT, 0), (ACROSS, 0)

    def dev(dx, flip):
        return lax.rem(chip + dx, chips) * CORES + lax.rem(core + flip, CORES)

    def seen_from(peer):
        return PEER_SLOT[((chips - peer[0]) % chips, peer[1])]

    loads = [pltpu.make_async_copy(hid_hbm.at[j], h_all.at[tile_id("own", 0, j)], load_sem.at[j]) for j in range(2)]
    loads.append(pltpu.make_async_copy(tgt_hbm, t_all.at[me], load_sem.at[2]))
    load_w = pltpu.make_async_copy(w_hbm, w_ref, load_sem.at[3])
    for load in loads:
        load.start()
    load_w.start()
    barrier = pltpu.get_barrier_semaphore()
    for peer in PEERS:
        pl.semaphore_signal(barrier, inc=1, device_id={"fsdp": dev(*peer)}, device_id_type=MESH)
    dw_ref[...] = jnp.zeros_like(dw_ref)
    lse_acc[...] = jnp.zeros_like(lse_acc)
    zt_acc[...] = jnp.zeros_like(zt_acc)

    fwd_chunks = chunks(rows, FWD_CHUNK)

    def z_store(buf, slot, chunk):
        start, size = fwd_chunks[chunk]
        return pltpu.make_async_copy(z_ref.at[buf, start:start + size], z_hbm.at[slot, start:start + size], z_out.at[buf, chunk])

    def z_load(buf, slot):
        return pltpu.make_async_copy(z_hbm.at[slot], z_ref.at[buf], z_back.at[buf])

    for chunk, (start, size) in enumerate(fwd_chunks):
        pltpu.make_async_copy(dw_ref.at[start:start + size], z_hbm.at[2 * groups, start:start + size], z_out.at[1, chunk]).start()
    for load in loads:
        load.wait()
    pl.semaphore_wait(barrier, len(PEERS))

    def gather_copy(owner, quarter, to):
        src_tile, src_part = place(owner, quarter)
        as_seen = ((owner[0] - to[0]) % chips, (owner[1] + to[1]) % CORES)
        dst_tile, dst_part = place(as_seen, quarter)
        idx = PEER_SLOT[as_seen] * 4 + quarter
        return pltpu.make_async_remote_copy(
            src_ref=h_all.at[src_tile, parts[src_part]], dst_ref=h_all.at[dst_tile, parts[dst_part]],
            send_sem=ag_send.at[idx], recv_sem=ag_recv.at[idx], device_id={"fsdp": dev(*to)}, device_id_type=MESH)

    def gather_recv(owner, quarter):
        dst_tile, dst_part = place(owner, quarter)
        idx = PEER_SLOT[owner] * 4 + quarter
        dst = h_all.at[dst_tile, parts[dst_part]]
        pltpu.make_async_remote_copy(
            src_ref=dst, dst_ref=dst, send_sem=ag_send.at[idx], recv_sem=ag_recv.at[idx],
            device_id={"fsdp": me}, device_id_type=MESH).wait_recv()

    for quarter in range(4):
        for to in (right, left, PARTNER):
            gather_copy(OWN, quarter, to).start()

    def target_copy(peer):
        slot = seen_from(peer)
        return pltpu.make_async_remote_copy(
            src_ref=t_all.at[me], dst_ref=t_all.at[me], send_sem=tgt_send.at[slot], recv_sem=tgt_recv.at[slot],
            device_id={"fsdp": dev(*peer)}, device_id_type=MESH)

    for peer in PEERS:
        target_copy(peer).start()
    load_w.wait()

    def pieces(tid):
        grp = lax.div(tid, 4)
        flip = lax.rem(lax.div(tid, 2), 2)
        j = lax.rem(tid, 2)
        mixed = lax.rem(lax.div(grp + 1, 2), 2)
        out = []
        for part in range(2):
            dx = mixed * (RIGHT, LEFT)[part] + lax.div(grp, 3) * ACROSS
            quarter = mixed * (2 * lax.div(grp, 2) + j) + (1 - mixed) * (2 * j + part)
            out.append((dev(dx, flip), quarter))
        return out

    def stat_copy(peer, block, quarter):
        return pltpu.make_async_remote_copy(
            src_ref=stat_loc.at[block, quarter], dst_ref=stat_in.at[seen_from(peer), block, quarter],
            send_sem=stat_send, recv_sem=stat_recv, device_id={"fsdp": dev(*peer)}, device_id_type=MESH)

    def fwd_tile(buf, tid):
        run_max = jnp.full((8, tile), -jnp.inf, F32)
        run_sum = jnp.zeros((8, tile), F32)
        for chunk, (start, size) in enumerate(fwd_chunks):
            sl = slice(start, start + size)
            z_ref[buf, sl, :] = lax.dot_general(
                w_ref[sl, :], h_all[tid], (((1,), (1,)), ((), ())), preferred_element_type=F32)
            z_grp = z_ref[buf, sl, :].reshape(size // 8, 8, tile)
            new_max = jnp.maximum(run_max, jnp.max(z_grp, axis=0))
            run_sum = run_sum * jnp.exp(run_max - new_max) + jnp.sum(jnp.exp(z_grp - new_max[None]), axis=0)
            run_max = new_max
            z_store(buf, tid, chunk).start()
        tot_max = jnp.max(run_max, axis=0, keepdims=True)
        tot_sum = jnp.sum(run_sum * jnp.exp(run_max - tot_max), axis=0, keepdims=True)
        for part, (block, quarter) in enumerate(pieces(tid)):
            lanes = slice(part * quarter_toks, (part + 1) * quarter_toks)
            stat_loc[block, quarter, 0] = tot_max[:, lanes]
            stat_loc[block, quarter, 1] = tot_sum[:, lanes]
        for block, quarter in pieces(tid):
            for peer in PEERS:
                stat_copy(peer, block, quarter).start()

    def fwd_pair(step, carry):
        @pl.when(step == 1)
        def _():
            for quarter in range(4):
                gather_recv(PARTNER, quarter)

        for late in range(2):
            @pl.when(step == 2 + 2 * late)
            def _():
                for quarter in (2 * late, 2 * late + 1):
                    for owner in (left, right):
                        gather_recv(owner, quarter)
                        if late == 0 and owner == left:
                            gather_copy(left, quarter, right).start()
                        if late == 1 and owner == right:
                            gather_copy(right, quarter, left).start()
                        gather_copy(owner, quarter, PARTNER).start()

            @pl.when(step == 3 + 2 * late)
            def _():
                for quarter in (2 * late, 2 * late + 1):
                    gather_recv((LEFT, 1), quarter)
                    gather_recv((RIGHT, 1), quarter)

        @pl.when(step == 6)
        def _():
            for quarter in range(4):
                gather_recv(across, quarter)
                gather_copy(across, quarter, PARTNER).start()

        @pl.when(step == 7)
        def _():
            for quarter in range(4):
                gather_recv((ACROSS, 1), quarter)

        @pl.when(step > 0)
        def _():
            for chunk in range(len(fwd_chunks)):
                z_store(0, 0, chunk).wait()

        fwd_tile(0, 2 * step)
        for chunk in range(len(fwd_chunks)):
            z_store(1, 0, chunk).wait()
        fwd_tile(1, 2 * step + 1)
        return carry

    lax.fori_loop(0, groups, fwd_pair, 0)

    for buf in range(2):
        for chunk in range(len(fwd_chunks)):
            z_store(buf, 0, chunk).wait()

    def pair_tile(pair, flip):
        return lax.rem(lax.shift_right_logical(jnp.int32(PAIR_CODE), 4 * pair), 16) + 2 * flip

    z_load(1, pair_tile(0, 0)).start()
    for peer in PEERS:
        target_copy(peer).wait_recv()
    all_stats = pltpu.make_async_remote_copy(
        src_ref=stat_in, dst_ref=stat_in, send_sem=stat_send, recv_sem=stat_recv, device_id={"fsdp": me}, device_id_type=MESH)
    all_stats.wait_recv()

    def d2d_copy(slot):
        return pltpu.make_async_remote_copy(
            src_ref=pbuf.at[slot], dst_ref=d2d_in.at[slot], send_sem=d2d_send.at[slot], recv_sem=d2d_recv.at[slot],
            device_id={"fsdp": dev(*PARTNER)}, device_id_type=MESH)

    def ici_copy(pair, part):
        kind, j = PAIRS[pair]
        if kind == "across":
            dst, recv = ring_in.at[part, j], ring_recv.at[part * 2 + j]
        else:
            dst, recv = fin_in.at[part, j // 2, parts[j % 2]], fin_recv.at[part * 4 + j]
        return pltpu.make_async_remote_copy(
            src_ref=pbuf.at[2 + pair % 4, parts[part]], dst_ref=dst, send_sem=ici_send.at[(pair % 4) * 2 + part], recv_sem=recv,
            device_id={"fsdp": dev(*(right, left)[part])}, device_id_type=MESH)

    def wait_ici_sends(slot):
        for part in range(2):
            pltpu.make_async_remote_copy(
                src_ref=pbuf.at[2 + slot, parts[part]], dst_ref=ring_in.at[0, 0], send_sem=ici_send.at[slot * 2 + part],
                recv_sem=ring_recv.at[0], device_id={"fsdp": me}, device_id_type=MESH).wait_send()

    def add_into(slot, base, count, sources):
        def body(i, carry):
            off = pl.multiple_of(i * 64, 64)
            sl = pl.ds(base + off, 64)
            tot = pbuf[slot, sl, :]
            for src in sources:
                tot = tot + src[pl.ds(off, 64), :]
            pbuf[slot, sl, :] = tot
            return carry
        lax.fori_loop(0, count // 64, body, 0)

    inv_tokens = 1.0 / tokens
    log_tokens = jnp.log(jnp.float32(tokens))
    bwd_chunks = chunks(rows, BWD_CHUNK)

    def bwd_tile(buf, slot, tid, with_dw):
        where = pieces(tid)

        stats = [stat_loc] + [stat_in.at[i] for i in range(len(PEERS))]
        maxes, sums = [
            [jnp.concatenate([ref[block, quarter, kind] for block, quarter in where], axis=1) for ref in stats] for kind in range(2)]
        tot_max = functools.reduce(jnp.maximum, maxes)
        tot_sum = sum(s * jnp.exp(m - tot_max) for m, s in zip(maxes, sums))
        lse = tot_max + jnp.log(tot_sum)
        lse_acc[...] += lse
        shift = lse + log_tokens
        tgt = jnp.concatenate([t_all[block, quarter] for block, quarter in where], axis=1) - me * rows
        zt_sum = zt_acc[...]
        for idx, (start, size) in enumerate(bwd_chunks):
            sl = slice(start, start + size)
            z = z_ref[buf, sl, :]
            mask = (lax.broadcasted_iota(jnp.int32, (size, tile), 0) + start) == tgt
            prob = jnp.exp(z - shift)
            dz_ref[buf, sl, :] = jnp.where(mask, prob - inv_tokens, prob).astype(BF16)
            zt_sum += jnp.sum(jnp.where(mask, z, 0.0).reshape(size // 8, 8, tile), axis=0)
            if with_dw:
                dw_ref[sl, :] += jnp.dot(dz_ref[buf, sl, :], h_all[tid], preferred_element_type=F32)
            dh_part = lax.dot_general(dz_ref[buf, sl, :], w_ref[sl, :], (((0,), (0,)), ((), ())), preferred_element_type=F32)
            if idx == 0:
                pbuf[slot] = dh_part
            else:
                pbuf[slot] += dh_part
        zt_acc[...] = zt_sum

    def finish_pair(pair):
        kind, j = PAIRS[pair]
        slot = 2 + pair % 4
        if kind == "own":
            for part in range(2):
                for q in range(2):
                    ici_copy(2 + 2 * j + q, part).wait_recv()
            add_into(slot, 0, tile, [d2d_in.at[pair % 2], fin_in.at[0, j], fin_in.at[1, j]])
            pltpu.make_async_copy(pbuf.at[slot], dh_hbm.at[j], out_sem.at[j]).start()
            return
        for part in range(2):
            sources = [d2d_in.at[pair % 2, parts[part]]]
            if kind == "mixed" and j % 2 == part:
                ici_copy(j // 2, part).wait_recv()
                sources.append(ring_in.at[part, j // 2])
            add_into(slot, part * quarter_toks, quarter_toks, sources)
            ici_copy(pair, part).start()

    def bwd_pair(pair, carry):
        odd = lax.rem(pair, 2)

        @pl.when(pair >= 2)
        def _():
            d2d_copy(odd).wait_send()

        @pl.when(pair >= 4)
        def _():
            wait_ici_sends(pair - 4)

        @pl.when(pair >= 1)
        def _():
            z_load(0, 0).wait()

        bwd_tile(0, odd, pair_tile(pair, 1), True)
        d2d_copy(odd).start()
        z_load(0, pair_tile(pair + 1, 1)).start()
        z_load(1, 0).wait()
        bwd_tile(1, 2 + lax.rem(pair, 4), pair_tile(pair, 0), True)
        z_load(1, pair_tile(pair + 1, 0)).start()
        d2d_copy(odd).wait_recv()
        for pair_s in range(len(PAIRS) - 1):
            @pl.when(pair == pair_s)
            def _():
                finish_pair(pair_s)
        return carry

    last = len(PAIRS) - 1
    lax.fori_loop(0, last, bwd_pair, 0)

    outs = [pltpu.make_async_copy(dw_ref, dw_hbm, out_sem.at[2])]
    outs += [pltpu.make_async_copy(h_all.at[tile_id("own", 1 - i, 1)], htail_hbm.at[i], out_sem.at[3 + i]) for i in range(2)]
    for out in outs:
        out.start()
    d2d_copy(last % 2).wait_send()
    wait_ici_sends(last - 4)
    for buf in range(2):
        z_load(buf, 0).wait()
        bwd_tile(buf, (last % 2, 2 + last % 4)[buf], tile_id("own", 1 - buf, 1), False)
        outs.append(pltpu.make_async_copy(dz_ref.at[buf], dz_hbm.at[buf], out_sem.at[5 + buf]))
        outs[-1].start()
        if buf == 0:
            d2d_copy(last % 2).start()

    zt_row[...] = jnp.sum(zt_acc[...], axis=0, keepdims=True)

    def zt_copy(peer):
        slot = seen_from(peer)
        return pltpu.make_async_remote_copy(
            src_ref=zt_row, dst_ref=zt_in.at[slot], send_sem=zt_send.at[slot], recv_sem=zt_recv.at[slot],
            device_id={"fsdp": dev(*peer)}, device_id_type=MESH)

    for peer in PEERS:
        zt_copy(peer).start()
    d2d_copy(last % 2).wait_recv()
    finish_pair(last)
    for peer in PEERS:
        zt_copy(peer).wait()
    tot = lse_acc[...] - zt_row[...]
    for i in range(len(PEERS)):
        tot = tot - zt_in[i]
    loss_ref[...] = jnp.broadcast_to(jnp.sum(tot, axis=1, keepdims=True) * inv_tokens, loss_ref.shape)

    for owner, quarter, to in (
            [(OWN, q, to) for q in range(4) for to in (right, left, PARTNER)]
            + [(left, q, right) for q in (0, 1)] + [(right, q, left) for q in (2, 3)]
            + [(side, q, PARTNER) for side in (left, right, across) for q in range(4)]):
        gather_copy(owner, quarter, to).wait_send()
    for peer in PEERS:
        target_copy(peer).wait_send()
    all_stats.wait_send()
    for slot in range(2):
        d2d_copy(slot).wait_send()
    for pair in (4, 5):
        wait_ici_sends(pair % 4)
    for j in range(2):
        pltpu.make_async_copy(pbuf.at[2 + (6 + j) % 4], dh_hbm.at[j], out_sem.at[j]).wait()
    for out in outs:
        out.wait()


def tail_kernel(dw_ref, dz_ref, h_ref, dh_ref, dw_out, dh_out):
    tot = dw_ref[...]
    for i in range(2):
        tot = tot + jnp.dot(dz_ref[i], h_ref[i], preferred_element_type=F32)
    dw_out[...] = tot
    dh_out[...] = dh_ref[...]


def solution(mesh):
    groups = mesh.shape["fsdp"]
    tok_spec = P(("dp", "fsdp"), None)

    def local_head(hidden, targets, weight):
        tok_loc, width = hidden.shape
        rows = weight.shape[0]
        tokens = tok_loc * groups
        tile, quarter = tok_loc // 2, tok_loc // 4
        peers = len(PEERS)
        any_spec = pl.BlockSpec(memory_space=pl.ANY)
        vmem, dma = pltpu.VMEM, pltpu.SemaphoreType.DMA
        shape = jax.ShapeDtypeStruct
        loss_row, grad_h, dw_part, dz_tail, h_tail, _ = pl.pallas_call(
            functools.partial(head_kernel, groups, tokens),
            in_specs=[any_spec] * 3,
            out_specs=[pl.BlockSpec(memory_space=pltpu.VMEM)] + [any_spec] * 5,
            out_shape=[
                shape((1, 128), F32), shape((2, tile, width), F32), shape((rows, width), F32), shape((2, rows, tile), BF16),
                shape((2, tile, width), BF16), shape((2 * groups + 1, rows, tile), F32)],
            scratch_shapes=[
                vmem((2 * groups, tile, width), BF16),
                vmem((groups, 4, 1, quarter), jnp.int32),
                vmem((rows, width), BF16),
                vmem((2, rows, tile), F32),
                vmem((2, rows, tile), BF16),
                vmem((rows, width), F32),
                vmem((6, tile, width), F32),
                vmem((2, tile, width), F32),
                vmem((2, 2, quarter, width), F32),
                vmem((2, 2, tile, width), F32),
                vmem((groups, 4, 2, 1, quarter), F32),
                vmem((peers, groups, 4, 2, 1, quarter), F32),
                vmem((1, tile), F32),
                vmem((8, tile), F32),
                vmem((1, tile), F32),
                vmem((peers, 1, tile), F32),
                dma((4,)), dma((4 * peers,)), dma((4 * peers,)), dma((peers,)), dma((peers,)), dma, dma,
                dma((2,)), dma((2,)), dma((8,)), dma((4,)), dma((8,)), dma((peers,)), dma((peers,)), dma((7,)),
                dma((2, len(chunks(rows, FWD_CHUNK)))), dma((2,)),
            ],
            compiler_params=pltpu.CompilerParams(collective_id=0, has_side_effects=True, vmem_limit_bytes=67_000_000),
            name="head",
        )(hidden.reshape(2, tile, width), targets.reshape(4, 1, quarter), weight)
        steps = pl.cdiv(rows, TAIL_ROWS)
        row_spec = pl.BlockSpec((TAIL_ROWS, width), lambda i: (i, 0))
        dh_spec = pl.BlockSpec((tok_loc // steps, width), lambda i: (i, 0))
        grad_w, grad_h = pl.pallas_call(
            tail_kernel,
            grid=(steps,),
            in_specs=[row_spec, pl.BlockSpec((2, TAIL_ROWS, tile), lambda i: (0, i, 0)),
                      pl.BlockSpec((2, tile, width), lambda i: (0, 0, 0)), dh_spec],
            out_specs=[row_spec, dh_spec],
            out_shape=[shape((rows, width), F32), shape((tok_loc, width), F32)],
            name="tail",
        )(dw_part, dz_tail, h_tail, grad_h.reshape(tok_loc, width))
        return loss_row[0, :1], grad_h, grad_w

    return jax.shard_map(local_head, mesh=mesh, in_specs=(tok_spec, P(("dp", "fsdp")), P("fsdp", None)), out_specs=(P("dp"), tok_spec, tok_spec), check_vma=False)
```

```python
import functools

import jax
import jax.numpy as jnp
from jax import lax
from jax.experimental import pallas as pl
from jax.experimental.pallas import tpu as pltpu
from jax.sharding import PartitionSpec as P

F32 = jnp.float32
BF16 = jnp.bfloat16
MESH = pl.DeviceIdType.MESH
CORES = 2
CHUNK = 1008
GROUP = 112
COPY_ROWS = 512

LEFT, RIGHT, ACROSS = 3, 1, 2
OWN, PARTNER = (0, 0), (0, 1)
PEERS = [PARTNER, (LEFT, 0), (LEFT, 1), (RIGHT, 0), (RIGHT, 1), (ACROSS, 0), (ACROSS, 1)]
PEER_SLOT = {peer: slot for slot, peer in enumerate(PEERS)}

def tile_id(kind, flip, j):
    if kind == "mixed":
        return 4 + 2 * flip + 4 * (j // 2) + j % 2
    return {"own": 0, "across": 12}[kind] + 2 * flip + j


def place(owner, quarter):
    dx, flip = owner
    if dx in (LEFT, RIGHT):
        return tile_id("mixed", flip, quarter), 0 if dx == RIGHT else 1
    return tile_id("own" if dx == 0 else "across", flip, quarter // 2), quarter % 2


PAIRS = [("across", 0), ("across", 1)] + [("mixed", j) for j in range(4)] + [("own", 0), ("own", 1)]
PAIR_CODE = sum(tile_id(kind, 0, j) << (4 * q) for q, (kind, j) in enumerate(PAIRS))


def chunks(rows, step):
    return [(start, min(step, rows - start)) for start in range(0, rows, step)]


def head_kernel(groups, tokens, hid_hbm, tgt_hbm, w_hbm, loss_ref, dh_hbm, dw_hbm, z_hbm,
                h_all, t_all, w_ref, z_ref, dz_ref, dw_ref, pbuf, d2d_in, ring_in, fin_in,
                stat_loc, stat_in, lse_acc, zt_acc, zt_row, zt_in,
                load_sem, ag_send, ag_recv, tgt_send, tgt_recv, stat_send, stat_recv,
                d2d_send, d2d_recv, ici_send, ring_recv, fin_recv, zt_send, zt_recv, out_sem, z_out, z_back):
    chips = groups // CORES
    me = lax.axis_index("fsdp")
    chip = lax.div(me, CORES)
    core = lax.rem(me, CORES)
    rows, width = w_ref.shape
    tile = h_all.shape[1]
    quarter_toks = tile // 2
    parts = [pl.ds(0, quarter_toks), pl.ds(quarter_toks, quarter_toks)]
    left, right, across = (LEFT, 0), (RIGHT, 0), (ACROSS, 0)

    def dev(dx, flip):
        return lax.rem(chip + dx, chips) * CORES + lax.rem(core + flip, CORES)

    def seen_from(peer):
        return PEER_SLOT[((chips - peer[0]) % chips, peer[1])]

    loads = [pltpu.make_async_copy(hid_hbm.at[j], h_all.at[tile_id("own", 0, j)], load_sem.at[j]) for j in range(2)]
    loads.append(pltpu.make_async_copy(tgt_hbm, t_all.at[me], load_sem.at[2]))
    load_w = pltpu.make_async_copy(w_hbm, w_ref, load_sem.at[3])
    for load in loads:
        load.start()
    load_w.start()
    barrier = pltpu.get_barrier_semaphore()
    for peer in PEERS:
        pl.semaphore_signal(barrier, inc=1, device_id={"fsdp": dev(*peer)}, device_id_type=MESH)
    dw_ref[...] = jnp.zeros_like(dw_ref)
    lse_acc[...] = jnp.zeros_like(lse_acc)
    zt_acc[...] = jnp.zeros_like(zt_acc)

    row_chunks = chunks(rows, CHUNK)

    def z_store(buf, slot, chunk):
        start, size = row_chunks[chunk]
        return pltpu.make_async_copy(z_ref.at[buf, start:start + size], z_hbm.at[slot, start:start + size], z_out.at[buf, chunk])

    def z_load(buf, slot):
        return pltpu.make_async_copy(z_hbm.at[slot], z_ref.at[buf], z_back.at[buf])

    for chunk, (start, size) in enumerate(row_chunks):
        pltpu.make_async_copy(dw_ref.at[start:start + size], z_hbm.at[2 * groups, start:start + size], z_out.at[1, chunk]).start()
    for load in loads:
        load.wait()
    pl.semaphore_wait(barrier, len(PEERS))

    def gather_copy(owner, quarter, to):
        src_tile, src_part = place(owner, quarter)
        as_seen = ((owner[0] - to[0]) % chips, (owner[1] + to[1]) % CORES)
        dst_tile, dst_part = place(as_seen, quarter)
        idx = PEER_SLOT[as_seen] * 4 + quarter
        return pltpu.make_async_remote_copy(
            src_ref=h_all.at[src_tile, parts[src_part]], dst_ref=h_all.at[dst_tile, parts[dst_part]],
            send_sem=ag_send.at[idx], recv_sem=ag_recv.at[idx], device_id={"fsdp": dev(*to)}, device_id_type=MESH)

    def gather_recv(owner, quarter):
        dst_tile, dst_part = place(owner, quarter)
        idx = PEER_SLOT[owner] * 4 + quarter
        dst = h_all.at[dst_tile, parts[dst_part]]
        pltpu.make_async_remote_copy(
            src_ref=dst, dst_ref=dst, send_sem=ag_send.at[idx], recv_sem=ag_recv.at[idx],
            device_id={"fsdp": me}, device_id_type=MESH).wait_recv()

    for quarter in range(4):
        for to in (right, left, PARTNER):
            gather_copy(OWN, quarter, to).start()

    def target_copy(peer):
        slot = seen_from(peer)
        return pltpu.make_async_remote_copy(
            src_ref=t_all.at[me], dst_ref=t_all.at[me], send_sem=tgt_send.at[slot], recv_sem=tgt_recv.at[slot],
            device_id={"fsdp": dev(*peer)}, device_id_type=MESH)

    for peer in PEERS:
        target_copy(peer).start()
    load_w.wait()

    def pieces(tid):
        grp = lax.div(tid, 4)
        flip = lax.rem(lax.div(tid, 2), 2)
        j = lax.rem(tid, 2)
        mixed = lax.rem(lax.div(grp + 1, 2), 2)
        out = []
        for part in range(2):
            dx = mixed * (RIGHT, LEFT)[part] + lax.div(grp, 3) * ACROSS
            quarter = mixed * (2 * lax.div(grp, 2) + j) + (1 - mixed) * (2 * j + part)
            out.append((dev(dx, flip), quarter))
        return out

    def stat_copy(peer, block, quarter):
        return pltpu.make_async_remote_copy(
            src_ref=stat_loc.at[block, quarter], dst_ref=stat_in.at[seen_from(peer), block, quarter],
            send_sem=stat_send, recv_sem=stat_recv, device_id={"fsdp": dev(*peer)}, device_id_type=MESH)

    def fwd_tile(buf, tid):
        run_max = jnp.full((8, tile), -jnp.inf, F32)
        run_sum = jnp.zeros((8, tile), F32)
        for chunk, (start, size) in enumerate(row_chunks):
            sl = slice(start, start + size)
            z_ref[buf, sl, :] = lax.dot_general(
                w_ref[sl, :], h_all[tid], (((1,), (1,)), ((), ())), preferred_element_type=F32)
            for first, count in chunks(size, GROUP):
                z_grp = z_ref[buf, start + first:start + first + count, :].reshape(count // 8, 8, tile)
                new_max = jnp.maximum(run_max, jnp.max(z_grp, axis=0))
                run_sum = run_sum * jnp.exp(run_max - new_max) + jnp.sum(jnp.exp(z_grp - new_max[None]), axis=0)
                run_max = new_max
            z_store(buf, tid, chunk).start()
        tot_max = jnp.max(run_max, axis=0, keepdims=True)
        tot_sum = jnp.sum(run_sum * jnp.exp(run_max - tot_max), axis=0, keepdims=True)
        for part, (block, quarter) in enumerate(pieces(tid)):
            lanes = slice(part * quarter_toks, (part + 1) * quarter_toks)
            stat_loc[block, quarter, 0] = tot_max[:, lanes]
            stat_loc[block, quarter, 1] = tot_sum[:, lanes]
        for block, quarter in pieces(tid):
            for peer in PEERS:
                stat_copy(peer, block, quarter).start()

    def fwd_pair(step, carry):
        @pl.when(step == 1)
        def _():
            for quarter in range(4):
                gather_recv(PARTNER, quarter)

        for late in range(2):
            @pl.when(step == 2 + 2 * late)
            def _():
                for quarter in (2 * late, 2 * late + 1):
                    for owner in (left, right):
                        gather_recv(owner, quarter)
                        if late == 0 and owner == left:
                            gather_copy(left, quarter, right).start()
                        if late == 1 and owner == right:
                            gather_copy(right, quarter, left).start()
                        gather_copy(owner, quarter, PARTNER).start()

            @pl.when(step == 3 + 2 * late)
            def _():
                for quarter in (2 * late, 2 * late + 1):
                    gather_recv((LEFT, 1), quarter)
                    gather_recv((RIGHT, 1), quarter)

        @pl.when(step == 6)
        def _():
            for quarter in range(4):
                gather_recv(across, quarter)
                gather_copy(across, quarter, PARTNER).start()

        @pl.when(step == 7)
        def _():
            for quarter in range(4):
                gather_recv((ACROSS, 1), quarter)

        @pl.when(step > 0)
        def _():
            for chunk in range(len(row_chunks)):
                z_store(0, 0, chunk).wait()

        fwd_tile(0, 2 * step)
        for chunk in range(len(row_chunks)):
            z_store(1, 0, chunk).wait()
        fwd_tile(1, 2 * step + 1)
        return carry

    lax.fori_loop(0, groups, fwd_pair, 0)

    for buf in range(2):
        for chunk in range(len(row_chunks)):
            z_store(buf, 0, chunk).wait()

    def pair_tile(pair, flip):
        return lax.rem(lax.shift_right_logical(jnp.int32(PAIR_CODE), 4 * pair), 16) + 2 * flip

    z_load(1, pair_tile(0, 0)).start()
    for peer in PEERS:
        target_copy(peer).wait_recv()
    all_stats = pltpu.make_async_remote_copy(
        src_ref=stat_in, dst_ref=stat_in, send_sem=stat_send, recv_sem=stat_recv, device_id={"fsdp": me}, device_id_type=MESH)
    all_stats.wait_recv()

    def d2d_copy(slot):
        return pltpu.make_async_remote_copy(
            src_ref=pbuf.at[slot], dst_ref=d2d_in.at[slot], send_sem=d2d_send.at[slot], recv_sem=d2d_recv.at[slot],
            device_id={"fsdp": dev(*PARTNER)}, device_id_type=MESH)

    def ici_copy(pair, part):
        kind, j = PAIRS[pair]
        if kind == "across":
            dst, recv = ring_in.at[part, j], ring_recv.at[part * 2 + j]
        else:
            dst, recv = fin_in.at[part, j // 2, parts[j % 2]], fin_recv.at[part * 4 + j]
        return pltpu.make_async_remote_copy(
            src_ref=pbuf.at[2 + pair % 4, parts[part]], dst_ref=dst, send_sem=ici_send.at[(pair % 4) * 2 + part], recv_sem=recv,
            device_id={"fsdp": dev(*(right, left)[part])}, device_id_type=MESH)

    def wait_ici_sends(slot):
        for part in range(2):
            pltpu.make_async_remote_copy(
                src_ref=pbuf.at[2 + slot, parts[part]], dst_ref=ring_in.at[0, 0], send_sem=ici_send.at[slot * 2 + part],
                recv_sem=ring_recv.at[0], device_id={"fsdp": me}, device_id_type=MESH).wait_send()

    def add_into(slot, base, count, sources):
        def body(i, carry):
            off = pl.multiple_of(i * 64, 64)
            sl = pl.ds(base + off, 64)
            tot = pbuf[slot, sl, :]
            for src in sources:
                tot = tot + src[pl.ds(off, 64), :]
            pbuf[slot, sl, :] = tot
            return carry
        lax.fori_loop(0, count // 64, body, 0)

    inv_tokens = 1.0 / tokens
    log_tokens = jnp.log(jnp.float32(tokens))

    def bwd_tile(buf, tid, dh_slot=None, with_dw=True, last=False):
        where = pieces(tid)
        stats = [stat_loc] + [stat_in.at[i] for i in range(len(PEERS))]
        maxes, sums = [
            [jnp.concatenate([ref[block, quarter, kind] for block, quarter in where], axis=1) for ref in stats] for kind in range(2)]
        tot_max = functools.reduce(jnp.maximum, maxes)
        tot_sum = sum(s * jnp.exp(m - tot_max) for m, s in zip(maxes, sums))
        lse = tot_max + jnp.log(tot_sum)
        shift = lse + log_tokens
        tgt = jnp.concatenate([t_all[block, quarter] for block, quarter in where], axis=1) - me * rows
        if dh_slot is not None:
            lse_acc[...] += lse
            zt_sum = zt_acc[...]
        for idx, (start, size) in enumerate(row_chunks):
            sl = slice(start, start + size)
            z = z_ref[buf, sl, :]
            mask = (lax.broadcasted_iota(jnp.int32, (size, tile), 0) + start) == tgt
            prob = jnp.exp(z - shift)
            dz_ref[sl, :] = jnp.where(mask, prob - inv_tokens, prob).astype(BF16)
            if with_dw:
                dw_ref[sl, :] += jnp.dot(dz_ref[sl, :], h_all[tid], preferred_element_type=F32)
            if last:
                dw_out(idx).start()
            if dh_slot is not None:
                zt_sum += jnp.sum(jnp.where(mask, z, 0.0).reshape(size // 8, 8, tile), axis=0)
                dh_part = lax.dot_general(dz_ref[sl, :], w_ref[sl, :], (((0,), (0,)), ((), ())), preferred_element_type=F32)
                if idx == 0:
                    pbuf[dh_slot] = dh_part
                else:
                    pbuf[dh_slot] += dh_part
        if dh_slot is not None:
            zt_acc[...] = zt_sum

    def dw_out(idx):
        start, size = row_chunks[idx]
        return pltpu.make_async_copy(dw_ref.at[start:start + size], dw_hbm.at[start:start + size], out_sem.at[2 + idx])

    def finish_pair(pair):
        kind, j = PAIRS[pair]
        slot = 2 + pair % 4
        if kind == "own":
            for part in range(2):
                for q in range(2):
                    ici_copy(2 + 2 * j + q, part).wait_recv()
            add_into(slot, 0, tile, [d2d_in.at[pair % 2], fin_in.at[0, j], fin_in.at[1, j]])
            pltpu.make_async_copy(pbuf.at[slot], dh_hbm.at[j], out_sem.at[j]).start()
            return
        for part in range(2):
            sources = [d2d_in.at[pair % 2, parts[part]]]
            if kind == "mixed" and j % 2 == part:
                ici_copy(j // 2, part).wait_recv()
                sources.append(ring_in.at[part, j // 2])
            add_into(slot, part * quarter_toks, quarter_toks, sources)
            ici_copy(pair, part).start()

    def run_pair(pair, odd, slot, with_dw):
        z_next = lax.rem(pair + 1, len(PAIRS))
        bwd_tile(0, pair_tile(pair, 1), odd, with_dw)
        d2d_copy(odd).start()
        z_load(0, pair_tile(z_next, 1)).start()
        z_load(1, 0).wait()
        bwd_tile(1, pair_tile(pair, 0), 2 + slot, with_dw)
        z_load(1, pair_tile(z_next, 0)).start()
        d2d_copy(odd).wait_recv()

    def bwd_pair(pair, carry):
        odd = lax.rem(pair, 2)

        @pl.when(pair >= 2)
        def _():
            d2d_copy(odd).wait_send()

        @pl.when(pair >= 4)
        def _():
            wait_ici_sends(pair - 4)

        z_load(0, 0).wait()
        run_pair(pair, odd, lax.rem(pair, 4), True)
        for pair_s in range(1, last):
            @pl.when(pair == pair_s)
            def _():
                finish_pair(pair_s)
        return carry

    last = len(PAIRS) - 1
    run_pair(jnp.int32(0), 0, 0, False)
    finish_pair(0)
    lax.fori_loop(1, last + 1, bwd_pair, 0)

    zt_row[...] = jnp.sum(zt_acc[...], axis=0, keepdims=True)

    def zt_copy(peer):
        slot = seen_from(peer)
        return pltpu.make_async_remote_copy(
            src_ref=zt_row, dst_ref=zt_in.at[slot], send_sem=zt_send.at[slot], recv_sem=zt_recv.at[slot],
            device_id={"fsdp": dev(*peer)}, device_id_type=MESH)

    for peer in PEERS:
        zt_copy(peer).start()
    for buf in range(2):
        z_load(buf, 0).wait()
        bwd_tile(buf, tile_id("across", 1 - buf, 0), last=buf == 1)
    finish_pair(last)
    for peer in PEERS:
        zt_copy(peer).wait()
    tot = lse_acc[...] - zt_row[...]
    for i in range(len(PEERS)):
        tot = tot - zt_in[i]
    loss_ref[...] = jnp.broadcast_to(jnp.sum(tot, axis=1, keepdims=True) * inv_tokens, loss_ref.shape)

    for owner, quarter, to in (
            [(OWN, q, to) for q in range(4) for to in (right, left, PARTNER)]
            + [(left, q, right) for q in (0, 1)] + [(right, q, left) for q in (2, 3)]
            + [(side, q, PARTNER) for side in (left, right, across) for q in range(4)]):
        gather_copy(owner, quarter, to).wait_send()
    for peer in PEERS:
        target_copy(peer).wait_send()
    all_stats.wait_send()
    for slot in range(2):
        d2d_copy(slot).wait_send()
    for pair in (4, 5):
        wait_ici_sends(pair % 4)
    for j in range(2):
        pltpu.make_async_copy(pbuf.at[2 + (6 + j) % 4], dh_hbm.at[j], out_sem.at[j]).wait()
    for idx in range(len(row_chunks)):
        dw_out(idx).wait()


def copy_kernel(dw_hbm, dh_hbm, dw_out, dh_out, dw_buf, dh_buf, in_sem, out_sem):
    moves = []
    for src, buf, dst in ((dw_hbm, dw_buf, dw_out), (dh_hbm, dh_buf, dh_out)):
        for start, size in chunks(src.shape[0], COPY_ROWS):
            sl = slice(start, start + size)
            moves.append((
                pltpu.make_async_copy(src.at[sl], buf.at[sl], in_sem.at[len(moves)]),
                pltpu.make_async_copy(buf.at[sl], dst.at[sl], out_sem.at[len(moves)])))
    for load, _ in moves:
        load.start()
    for load, store in moves:
        load.wait()
        store.start()
    for _, store in moves:
        store.wait()


def solution(mesh):
    groups = mesh.shape["fsdp"]
    tok_spec = P(("dp", "fsdp"), None)

    def local_head(hidden, targets, weight):
        tok_loc, width = hidden.shape
        rows = weight.shape[0]
        tokens = tok_loc * groups
        tile, quarter = tok_loc // 2, tok_loc // 4
        peers = len(PEERS)
        any_spec = pl.BlockSpec(memory_space=pl.ANY)
        vmem, dma = pltpu.VMEM, pltpu.SemaphoreType.DMA
        shape = jax.ShapeDtypeStruct
        loss_row, grad_h, grad_w, _ = pl.pallas_call(
            functools.partial(head_kernel, groups, tokens),
            in_specs=[any_spec] * 3,
            out_specs=[pl.BlockSpec(memory_space=pltpu.VMEM)] + [any_spec] * 3,
            out_shape=[
                shape((1, 128), F32), shape((2, tile, width), F32), shape((rows, width), F32), shape((2 * groups + 1, rows, tile), F32)],
            scratch_shapes=[
                vmem((2 * groups, tile, width), BF16),
                vmem((groups, 4, 1, quarter), jnp.int32),
                vmem((rows, width), BF16),
                vmem((2, rows, tile), F32),
                vmem((rows, tile), BF16),
                vmem((rows, width), F32),
                vmem((6, tile, width), F32),
                vmem((2, tile, width), F32),
                vmem((2, 2, quarter, width), F32),
                vmem((2, 2, tile, width), F32),
                vmem((groups, 4, 2, 1, quarter), F32),
                vmem((peers, groups, 4, 2, 1, quarter), F32),
                vmem((1, tile), F32),
                vmem((8, tile), F32),
                vmem((1, tile), F32),
                vmem((peers, 1, tile), F32),
                dma((4,)), dma((4 * peers,)), dma((4 * peers,)), dma((peers,)), dma((peers,)), dma, dma,
                dma((2,)), dma((2,)), dma((8,)), dma((4,)), dma((8,)), dma((peers,)), dma((peers,)), dma((2 + len(chunks(rows, CHUNK)),)),
                dma((2, len(chunks(rows, CHUNK)))), dma((2,)),
            ],
            compiler_params=pltpu.CompilerParams(collective_id=0, has_side_effects=True, vmem_limit_bytes=67_000_000),
            name="head",
        )(hidden.reshape(2, tile, width), targets.reshape(4, 1, quarter), weight)
        copies = len(chunks(rows, COPY_ROWS)) + len(chunks(tok_loc, COPY_ROWS))
        grad_w, grad_h = pl.pallas_call(
            copy_kernel,
            in_specs=[any_spec] * 2,
            out_specs=[any_spec] * 2,
            out_shape=[shape((rows, width), F32), shape((tok_loc, width), F32)],
            scratch_shapes=[vmem((rows, width), F32), vmem((tok_loc, width), F32), dma((copies,)), dma((copies,))],
            name="results",
        )(grad_w, grad_h.reshape(tok_loc, width))
        return loss_row[0, :1], grad_h, grad_w

    return jax.shard_map(local_head, mesh=mesh, in_specs=(tok_spec, P(("dp", "fsdp")), P("fsdp", None)), out_specs=(P("dp"), tok_spec, tok_spec), check_vma=False)
```

```python
import functools

import jax
import jax.numpy as jnp
from jax import lax
from jax.experimental import pallas as pl
from jax.experimental.pallas import tpu as pltpu
from jax.sharding import PartitionSpec as P

F32 = jnp.float32
BF16 = jnp.bfloat16
MESH = pl.DeviceIdType.MESH
CORES = 2
CHUNK = 1008
GROUP = 112
COPY_ROWS = 512

LEFT, RIGHT, ACROSS = 3, 1, 2
OWN, PARTNER = (0, 0), (0, 1)
PEERS = [PARTNER, (LEFT, 0), (LEFT, 1), (RIGHT, 0), (RIGHT, 1), (ACROSS, 0), (ACROSS, 1)]
PEER_SLOT = {peer: slot for slot, peer in enumerate(PEERS)}

def tile_id(kind, flip, j):
    if kind == "own":
        return 2 * flip + j
    return {"mixed": 4, "across": 12}[kind] + 2 * j + flip


def place(owner, quarter):
    dx, flip = owner
    if dx in (LEFT, RIGHT):
        return tile_id("mixed", flip, quarter), 0 if dx == RIGHT else 1
    if dx == ACROSS:
        return tile_id("across", flip, quarter % 2), quarter // 2
    return tile_id("own", flip, quarter // 2), quarter % 2


PAIRS = [("across", 0), ("across", 1)] + [("mixed", j) for j in range(4)] + [("own", 0), ("own", 1)]
PAIR_CODE = sum(tile_id(kind, 0, j) << (4 * q) for q, (kind, j) in enumerate(PAIRS))


def chunks(rows, step):
    return [(start, min(step, rows - start)) for start in range(0, rows, step)]


def head_kernel(groups, tokens, hid_hbm, tgt_hbm, w_hbm, loss_ref, dh_hbm, dw_hbm, z_hbm,
                h_all, t_all, w_ref, z_ref, dz_ref, dw_ref, pbuf, d2d_in, ring_in, fin_in,
                stat_loc, stat_in, lse_acc, zt_acc, zt_row, zt_in,
                load_sem, ag_send, ag_recv, tgt_send, tgt_recv, stat_send, stat_recv,
                d2d_send, d2d_recv, ici_send, ring_recv, fin_recv, zt_send, zt_recv, out_sem, z_out, z_back):
    chips = groups // CORES
    me = lax.axis_index("fsdp")
    chip = lax.div(me, CORES)
    core = lax.rem(me, CORES)
    rows, width = w_ref.shape
    tile = h_all.shape[1]
    quarter_toks = tile // 2
    parts = [pl.ds(0, quarter_toks), pl.ds(quarter_toks, quarter_toks)]
    left, right, across = (LEFT, 0), (RIGHT, 0), (ACROSS, 0)

    def dev(dx, flip):
        return lax.rem(chip + dx, chips) * CORES + lax.rem(core + flip, CORES)

    def seen_from(peer):
        return PEER_SLOT[((chips - peer[0]) % chips, peer[1])]

    loads = [pltpu.make_async_copy(hid_hbm.at[j], h_all.at[tile_id("own", 0, j)], load_sem.at[j]) for j in range(2)]
    loads.append(pltpu.make_async_copy(tgt_hbm, t_all.at[me], load_sem.at[2]))
    load_w = pltpu.make_async_copy(w_hbm, w_ref, load_sem.at[3])
    for load in loads:
        load.start()
    load_w.start()
    barrier = pltpu.get_barrier_semaphore()
    for peer in PEERS:
        pl.semaphore_signal(barrier, inc=1, device_id={"fsdp": dev(*peer)}, device_id_type=MESH)
    dw_ref[...] = jnp.zeros_like(dw_ref)
    lse_acc[...] = jnp.zeros_like(lse_acc)
    zt_acc[...] = jnp.zeros_like(zt_acc)

    row_chunks = chunks(rows, CHUNK)

    def z_store(buf, slot, chunk):
        start, size = row_chunks[chunk]
        return pltpu.make_async_copy(z_ref.at[buf, start:start + size], z_hbm.at[slot, start:start + size], z_out.at[buf, chunk])

    def z_load(buf, slot):
        return pltpu.make_async_copy(z_hbm.at[slot], z_ref.at[buf], z_back.at[buf])

    for chunk, (start, size) in enumerate(row_chunks):
        pltpu.make_async_copy(dw_ref.at[start:start + size], z_hbm.at[2 * groups, start:start + size], z_out.at[1, chunk]).start()
    for load in loads:
        load.wait()
    pl.semaphore_wait(barrier, len(PEERS))

    def gather_copy(owner, quarter, to):
        src_tile, src_part = place(owner, quarter)
        as_seen = ((owner[0] - to[0]) % chips, (owner[1] + to[1]) % CORES)
        dst_tile, dst_part = place(as_seen, quarter)
        idx = PEER_SLOT[as_seen] * 4 + quarter
        return pltpu.make_async_remote_copy(
            src_ref=h_all.at[src_tile, parts[src_part]], dst_ref=h_all.at[dst_tile, parts[dst_part]],
            send_sem=ag_send.at[idx], recv_sem=ag_recv.at[idx], device_id={"fsdp": dev(*to)}, device_id_type=MESH)

    def gather_recv(owner, quarter):
        dst_tile, dst_part = place(owner, quarter)
        idx = PEER_SLOT[owner] * 4 + quarter
        dst = h_all.at[dst_tile, parts[dst_part]]
        pltpu.make_async_remote_copy(
            src_ref=dst, dst_ref=dst, send_sem=ag_send.at[idx], recv_sem=ag_recv.at[idx],
            device_id={"fsdp": me}, device_id_type=MESH).wait_recv()

    for quarter in range(4):
        for to in (right, left, PARTNER):
            gather_copy(OWN, quarter, to).start()

    def target_copy(peer):
        slot = seen_from(peer)
        return pltpu.make_async_remote_copy(
            src_ref=t_all.at[me], dst_ref=t_all.at[me], send_sem=tgt_send.at[slot], recv_sem=tgt_recv.at[slot],
            device_id={"fsdp": dev(*peer)}, device_id_type=MESH)

    for peer in PEERS:
        target_copy(peer).start()
    load_w.wait()

    def pieces(tid):
        step, sub = lax.div(tid, 2), lax.rem(tid, 2)
        is_own = 1 - lax.div(lax.div(step, 2) + 3, 4)
        is_across = lax.div(step, 6)
        mixed = 1 - is_own - is_across
        flip = is_own * step + (1 - is_own) * sub
        j = is_own * sub + (1 - is_own) * (step - 2 - 4 * is_across)
        out = []
        for part in range(2):
            dx = mixed * (RIGHT, LEFT)[part] + is_across * ACROSS
            quarter = mixed * j + is_own * (2 * j + part) + is_across * (j + 2 * part)
            out.append((dev(dx, flip), quarter))
        return out

    def stat_copy(peer, block):
        return pltpu.make_async_remote_copy(
            src_ref=stat_loc.at[block], dst_ref=stat_in.at[seen_from(peer), block],
            send_sem=stat_send, recv_sem=stat_recv, device_id={"fsdp": dev(*peer)}, device_id_type=MESH)

    def fwd_tile(buf, tid):
        run_max = jnp.full((8, tile), -jnp.inf, F32)
        run_sum = jnp.zeros((8, tile), F32)
        for chunk, (start, size) in enumerate(row_chunks):
            sl = slice(start, start + size)
            z_ref[buf, sl, :] = lax.dot_general(
                w_ref[sl, :], h_all[tid], (((1,), (1,)), ((), ())), preferred_element_type=F32)
            for first, count in chunks(size, GROUP):
                z_grp = z_ref[buf, start + first:start + first + count, :].reshape(count // 8, 8, tile)
                new_max = jnp.maximum(run_max, jnp.max(z_grp, axis=0))
                run_sum = run_sum * jnp.exp(run_max - new_max) + jnp.sum(jnp.exp(z_grp - new_max[None]), axis=0)
                run_max = new_max
            z_store(buf, tid, chunk).start()
        tot_max = jnp.max(run_max, axis=0, keepdims=True)
        tot_sum = jnp.sum(run_sum * jnp.exp(run_max - tot_max), axis=0, keepdims=True)
        for part, (block, quarter) in enumerate(pieces(tid)):
            lanes = slice(part * quarter_toks, (part + 1) * quarter_toks)
            stat_loc[block, quarter, 0] = tot_max[:, lanes]
            stat_loc[block, quarter, 1] = tot_sum[:, lanes]

    def fwd_pair(step, carry):
        @pl.when(step == 1)
        def _():
            for quarter in range(4):
                gather_recv(PARTNER, quarter)

        for j in range(4):
            @pl.when(step == 2 + j)
            def _():
                gather_recv(left, j)
                gather_recv(right, j)
                if j < 2:
                    gather_copy(left, j, right).start()
                else:
                    gather_copy(right, j, left).start()
                gather_copy(left, j, PARTNER).start()
                gather_copy(right, j, PARTNER).start()

        for j in range(2):
            @pl.when(step == 6 + j)
            def _():
                if j == 0:
                    for owner in [OWN] + PEERS[:5]:
                        for peer in PEERS:
                            stat_copy(peer, dev(*owner)).start()
                for quarter in (j, j + 2):
                    gather_recv(across, quarter)
                    gather_copy(across, quarter, PARTNER).start()

        @pl.when(step > 0)
        def _():
            for chunk in range(len(row_chunks)):
                z_store(0, 0, chunk).wait()

        fwd_tile(0, 2 * step)
        for j in range(4):
            @pl.when(step == 2 + j)
            def _():
                gather_recv((LEFT, 1), j)
                gather_recv((RIGHT, 1), j)

        for j in range(2):
            @pl.when(step == 6 + j)
            def _():
                gather_recv((ACROSS, 1), j)
                gather_recv((ACROSS, 1), j + 2)

        for chunk in range(len(row_chunks)):
            z_store(1, 0, chunk).wait()
        fwd_tile(1, 2 * step + 1)
        return carry

    lax.fori_loop(0, groups, fwd_pair, 0)

    for owner in PEERS[5:]:
        for peer in PEERS:
            stat_copy(peer, dev(*owner)).start()

    def pair_tile(pair, flip):
        return lax.rem(lax.shift_right_logical(jnp.int32(PAIR_CODE), 4 * pair), 16) + flip * (1 + lax.div(pair, 6))

    for buf in range(2):
        for chunk in range(len(row_chunks)):
            z_store(buf, 0, chunk).wait()
        z_load(buf, tile_id("across", 1 - buf, 0)).start()
    for peer in PEERS:
        target_copy(peer).wait_recv()
    all_stats = pltpu.make_async_remote_copy(
        src_ref=stat_in, dst_ref=stat_in, send_sem=stat_send, recv_sem=stat_recv, device_id={"fsdp": me}, device_id_type=MESH)
    all_stats.wait_recv()

    def d2d_copy(slot):
        return pltpu.make_async_remote_copy(
            src_ref=pbuf.at[slot], dst_ref=d2d_in.at[slot], send_sem=d2d_send.at[slot], recv_sem=d2d_recv.at[slot],
            device_id={"fsdp": dev(*PARTNER)}, device_id_type=MESH)

    def ici_copy(pair, part):
        kind, j = PAIRS[pair]
        if kind == "across":
            dst, recv = ring_in.at[part, j], ring_recv.at[part * 2 + j]
        else:
            dst, recv = fin_in.at[part, j // 2, parts[j % 2]], fin_recv.at[part * 4 + j]
        return pltpu.make_async_remote_copy(
            src_ref=pbuf.at[2 + pair % 4, parts[part]], dst_ref=dst, send_sem=ici_send.at[(pair % 4) * 2 + part], recv_sem=recv,
            device_id={"fsdp": dev(*(right, left)[part])}, device_id_type=MESH)

    def wait_ici_sends(slot):
        for part in range(2):
            pltpu.make_async_remote_copy(
                src_ref=pbuf.at[2 + slot, parts[part]], dst_ref=ring_in.at[0, 0], send_sem=ici_send.at[slot * 2 + part],
                recv_sem=ring_recv.at[0], device_id={"fsdp": me}, device_id_type=MESH).wait_send()

    def add_into(slot, base, count, sources):
        def body(i, carry):
            off = pl.multiple_of(i * 64, 64)
            sl = pl.ds(base + off, 64)
            tot = pbuf[slot, sl, :]
            for src in sources:
                tot = tot + src[pl.ds(off, 64), :]
            pbuf[slot, sl, :] = tot
            return carry
        lax.fori_loop(0, count // 64, body, 0)

    inv_tokens = 1.0 / tokens
    log_tokens = jnp.log(jnp.float32(tokens))

    def bwd_tile(buf, tid, dh_slot=None, with_dw=True, last=False):
        where = pieces(tid)
        stats = [stat_loc] + [stat_in.at[i] for i in range(len(PEERS))]
        maxes, sums = [
            [jnp.concatenate([ref[block, quarter, kind] for block, quarter in where], axis=1) for ref in stats] for kind in range(2)]
        tot_max = functools.reduce(jnp.maximum, maxes)
        tot_sum = sum(s * jnp.exp(m - tot_max) for m, s in zip(maxes, sums))
        lse = tot_max + jnp.log(tot_sum)
        shift = lse + log_tokens
        tgt = jnp.concatenate([t_all[block, quarter] for block, quarter in where], axis=1) - me * rows
        if dh_slot is not None:
            lse_acc[...] += lse
            zt_sum = zt_acc[...]
        for idx, (start, size) in enumerate(row_chunks):
            sl = slice(start, start + size)
            z = z_ref[buf, sl, :]
            mask = (lax.broadcasted_iota(jnp.int32, (size, tile), 0) + start) == tgt
            prob = jnp.exp(z - shift)
            dz_ref[sl, :] = jnp.where(mask, prob - inv_tokens, prob).astype(BF16)
            if with_dw:
                dw_ref[sl, :] += jnp.dot(dz_ref[sl, :], h_all[tid], preferred_element_type=F32)
            if last:
                dw_out(idx).start()
            if dh_slot is not None:
                zt_sum += jnp.sum(jnp.where(mask, z, 0.0).reshape(size // 8, 8, tile), axis=0)
                dh_part = lax.dot_general(dz_ref[sl, :], w_ref[sl, :], (((0,), (0,)), ((), ())), preferred_element_type=F32)
                if idx == 0:
                    pbuf[dh_slot] = dh_part
                else:
                    pbuf[dh_slot] += dh_part
        if dh_slot is not None:
            zt_acc[...] = zt_sum

    def dw_out(idx):
        start, size = row_chunks[idx]
        return pltpu.make_async_copy(dw_ref.at[start:start + size], dw_hbm.at[start:start + size], out_sem.at[2 + idx])

    def finish_pair(pair):
        kind, j = PAIRS[pair]
        slot = 2 + pair % 4
        if kind == "own":
            for part in range(2):
                for q in range(2):
                    ici_copy(2 + 2 * j + q, part).wait_recv()
            add_into(slot, 0, tile, [d2d_in.at[pair % 2], fin_in.at[0, j], fin_in.at[1, j]])
            pltpu.make_async_copy(pbuf.at[slot], dh_hbm.at[j], out_sem.at[j]).start()
            return
        for part in range(2):
            sources = [d2d_in.at[pair % 2, parts[part]]]
            if kind == "mixed" and j // 2 == part:
                ici_copy(j % 2, part).wait_recv()
                sources.append(ring_in.at[part, j % 2])
            add_into(slot, part * quarter_toks, quarter_toks, sources)
            ici_copy(pair, part).start()

    def run_pair(pair, odd, slot, with_dw):
        z_next = lax.rem(pair + 1, len(PAIRS))
        bwd_tile(0, pair_tile(pair, 1), odd, with_dw)
        d2d_copy(odd).start()
        z_load(0, pair_tile(z_next, 1)).start()
        z_load(1, 0).wait()
        bwd_tile(1, pair_tile(pair, 0), 2 + slot, with_dw)
        z_load(1, pair_tile(z_next, 0)).start()
        d2d_copy(odd).wait_recv()

    def bwd_pair(pair, carry):
        odd = lax.rem(pair, 2)

        @pl.when(pair >= 2)
        def _():
            d2d_copy(odd).wait_send()

        @pl.when(pair >= 4)
        def _():
            wait_ici_sends(pair - 4)

        z_load(0, 0).wait()
        run_pair(pair, odd, lax.rem(pair, 4), True)
        for pair_s in range(1, last):
            @pl.when(pair == pair_s)
            def _():
                finish_pair(pair_s)
        return carry

    last = len(PAIRS) - 1
    z_load(0, 0).wait()
    run_pair(jnp.int32(0), 0, 0, False)
    finish_pair(0)
    lax.fori_loop(1, last + 1, bwd_pair, 0)

    zt_row[...] = jnp.sum(zt_acc[...], axis=0, keepdims=True)

    def zt_copy(peer):
        slot = seen_from(peer)
        return pltpu.make_async_remote_copy(
            src_ref=zt_row, dst_ref=zt_in.at[slot], send_sem=zt_send.at[slot], recv_sem=zt_recv.at[slot],
            device_id={"fsdp": dev(*peer)}, device_id_type=MESH)

    for peer in PEERS:
        zt_copy(peer).start()
    for buf in range(2):
        z_load(buf, 0).wait()
        bwd_tile(buf, tile_id("across", 1 - buf, 0), last=buf == 1)
    finish_pair(last)
    for peer in PEERS:
        zt_copy(peer).wait()
    tot = lse_acc[...] - zt_row[...]
    for i in range(len(PEERS)):
        tot = tot - zt_in[i]
    loss_ref[...] = jnp.broadcast_to(jnp.sum(tot, axis=1, keepdims=True) * inv_tokens, loss_ref.shape)

    for owner, quarter, to in (
            [(OWN, q, to) for q in range(4) for to in (right, left, PARTNER)]
            + [(left, q, right) for q in (0, 1)] + [(right, q, left) for q in (2, 3)]
            + [(side, q, PARTNER) for side in (left, right, across) for q in range(4)]):
        gather_copy(owner, quarter, to).wait_send()
    for peer in PEERS:
        target_copy(peer).wait_send()
    all_stats.wait_send()
    for slot in range(2):
        d2d_copy(slot).wait_send()
    for pair in (4, 5):
        wait_ici_sends(pair % 4)
    for j in range(2):
        pltpu.make_async_copy(pbuf.at[2 + (6 + j) % 4], dh_hbm.at[j], out_sem.at[j]).wait()
    for idx in range(len(row_chunks)):
        dw_out(idx).wait()


def copy_kernel(dw_hbm, dh_hbm, dw_out, dh_out, dw_buf, dh_buf, in_sem, out_sem):
    moves = []
    for src, buf, dst in ((dw_hbm, dw_buf, dw_out), (dh_hbm, dh_buf, dh_out)):
        for start, size in chunks(src.shape[0], COPY_ROWS):
            sl = slice(start, start + size)
            moves.append((
                pltpu.make_async_copy(src.at[sl], buf.at[sl], in_sem.at[len(moves)]),
                pltpu.make_async_copy(buf.at[sl], dst.at[sl], out_sem.at[len(moves)])))
    for load, _ in moves:
        load.start()
    for load, store in moves:
        load.wait()
        store.start()
    for _, store in moves:
        store.wait()


def solution(mesh):
    groups = mesh.shape["fsdp"]
    tok_spec = P(("dp", "fsdp"), None)

    def local_head(hidden, targets, weight):
        tok_loc, width = hidden.shape
        rows = weight.shape[0]
        tokens = tok_loc * groups
        tile, quarter = tok_loc // 2, tok_loc // 4
        peers = len(PEERS)
        any_spec = pl.BlockSpec(memory_space=pl.ANY)
        vmem, dma = pltpu.VMEM, pltpu.SemaphoreType.DMA
        shape = jax.ShapeDtypeStruct
        loss_row, grad_h, grad_w, _ = pl.pallas_call(
            functools.partial(head_kernel, groups, tokens),
            in_specs=[any_spec] * 3,
            out_specs=[pl.BlockSpec(memory_space=pltpu.VMEM)] + [any_spec] * 3,
            out_shape=[
                shape((1, 128), F32), shape((2, tile, width), F32), shape((rows, width), F32), shape((2 * groups + 1, rows, tile), F32)],
            scratch_shapes=[
                vmem((2 * groups, tile, width), BF16),
                vmem((groups, 4, 1, quarter), jnp.int32),
                vmem((rows, width), BF16),
                vmem((2, rows, tile), F32),
                vmem((rows, tile), BF16),
                vmem((rows, width), F32),
                vmem((6, tile, width), F32),
                vmem((2, tile, width), F32),
                vmem((2, 2, quarter, width), F32),
                vmem((2, 2, tile, width), F32),
                vmem((groups, 4, 2, 1, quarter), F32),
                vmem((peers, groups, 4, 2, 1, quarter), F32),
                vmem((1, tile), F32),
                vmem((8, tile), F32),
                vmem((1, tile), F32),
                vmem((peers, 1, tile), F32),
                dma((4,)), dma((4 * peers,)), dma((4 * peers,)), dma((peers,)), dma((peers,)), dma, dma,
                dma((2,)), dma((2,)), dma((8,)), dma((4,)), dma((8,)), dma((peers,)), dma((peers,)), dma((2 + len(chunks(rows, CHUNK)),)),
                dma((2, len(chunks(rows, CHUNK)))), dma((2,)),
            ],
            compiler_params=pltpu.CompilerParams(collective_id=0, has_side_effects=True, vmem_limit_bytes=67_000_000),
            name="head",
        )(hidden.reshape(2, tile, width), targets.reshape(4, 1, quarter), weight)
        copies = len(chunks(rows, COPY_ROWS)) + len(chunks(tok_loc, COPY_ROWS))
        grad_w, grad_h = pl.pallas_call(
            copy_kernel,
            in_specs=[any_spec] * 2,
            out_specs=[any_spec] * 2,
            out_shape=[shape((rows, width), F32), shape((tok_loc, width), F32)],
            scratch_shapes=[vmem((rows, width), F32), vmem((tok_loc, width), F32), dma((copies,)), dma((copies,))],
            name="results",
        )(grad_w, grad_h.reshape(tok_loc, width))
        return loss_row[0, :1], grad_h, grad_w

    return jax.shard_map(local_head, mesh=mesh, in_specs=(tok_spec, P(("dp", "fsdp")), P("fsdp", None)), out_specs=(P("dp"), tok_spec, tok_spec), check_vma=False)
```

```python
import functools

import jax
import jax.numpy as jnp
from jax import lax
from jax.experimental import pallas as pl
from jax.experimental.pallas import tpu as pltpu
from jax.sharding import PartitionSpec as P

F32 = jnp.float32
BF16 = jnp.bfloat16
MESH = pl.DeviceIdType.MESH
CORES = 2
CHUNK = 1008
GROUP = 112
SUMS = 3
VMEM_LIMIT = 56_000_000

LEFT, RIGHT, ACROSS = 3, 1, 2
OWN, PARTNER = (0, 0), (0, 1)
PEERS = [PARTNER, (LEFT, 0), (LEFT, 1), (RIGHT, 0), (RIGHT, 1), (ACROSS, 0), (ACROSS, 1)]
PEER_SLOT = {peer: slot for slot, peer in enumerate(PEERS)}

def tile_id(kind, flip, j):
    if kind == "own":
        return 2 * flip + j
    return {"mixed": 4, "across": 12}[kind] + 2 * j + flip


def place(owner, quarter):
    dx, flip = owner
    if dx in (LEFT, RIGHT):
        return tile_id("mixed", flip, quarter), 0 if dx == RIGHT else 1
    if dx == ACROSS:
        return tile_id("across", flip, quarter % 2), quarter // 2
    return tile_id("own", flip, quarter // 2), quarter % 2


PAIRS = [("across", 0), ("across", 1)] + [("mixed", j) for j in range(4)] + [("own", 0), ("own", 1)]
PAIR_CODE = sum(tile_id(kind, 0, j) << (4 * q) for q, (kind, j) in enumerate(PAIRS))


def chunks(rows, step):
    return [(start, min(step, rows - start)) for start in range(0, rows, step)]


def head_kernel(groups, tokens, hid_hbm, tgt_hbm, w_hbm, loss_ref, dh_ref, dw_ref, z_hbm,
                h_all, t_all, w_ref, z_ref, dz_ref, pbuf, d2d_in, ring_in, fin_in,
                stat_loc, stat_in, lse_acc, zt_acc, zt_row, zt_in,
                load_sem, ag_send, ag_recv, tgt_send, tgt_recv, stat_send, stat_recv,
                d2d_send, d2d_recv, ici_send, ring_recv, fin_recv, zt_send, zt_recv, z_out, z_back):
    chips = groups // CORES
    me = lax.axis_index("fsdp")
    chip = lax.div(me, CORES)
    core = lax.rem(me, CORES)
    rows, width = w_ref.shape
    tile = h_all.shape[1]
    quarter_toks = tile // 2
    parts = [pl.ds(0, quarter_toks), pl.ds(quarter_toks, quarter_toks)]
    left, right, across = (LEFT, 0), (RIGHT, 0), (ACROSS, 0)

    def dev(dx, flip):
        return lax.rem(chip + dx, chips) * CORES + lax.rem(core + flip, CORES)

    def seen_from(peer):
        return PEER_SLOT[((chips - peer[0]) % chips, peer[1])]

    loads = [pltpu.make_async_copy(hid_hbm.at[j], h_all.at[tile_id("own", 0, j)], load_sem.at[j]) for j in range(2)]
    loads.append(pltpu.make_async_copy(tgt_hbm, t_all.at[me], load_sem.at[2]))
    load_w = pltpu.make_async_copy(w_hbm, w_ref, load_sem.at[3])
    for load in loads:
        load.start()
    load_w.start()
    barrier = pltpu.get_barrier_semaphore()
    for peer in PEERS:
        pl.semaphore_signal(barrier, inc=1, device_id={"fsdp": dev(*peer)}, device_id_type=MESH)
    dw_ref[...] = jnp.zeros_like(dw_ref)
    lse_acc[...] = jnp.zeros_like(lse_acc)
    zt_acc[...] = jnp.zeros_like(zt_acc)

    row_chunks = chunks(rows, CHUNK)

    def z_store(buf, slot, chunk):
        start, size = row_chunks[chunk]
        return pltpu.make_async_copy(z_ref.at[buf, start:start + size], z_hbm.at[slot, start:start + size], z_out.at[buf, chunk])

    def z_load(buf, slot):
        return pltpu.make_async_copy(z_hbm.at[slot], z_ref.at[buf], z_back.at[buf])

    for chunk, (start, size) in enumerate(row_chunks):
        pltpu.make_async_copy(dw_ref.at[start:start + size], z_hbm.at[2 * groups, start:start + size], z_out.at[1, chunk]).start()
    for load in loads:
        load.wait()
    pl.semaphore_wait(barrier, len(PEERS))

    def gather_copy(owner, quarter, to):
        src_tile, src_part = place(owner, quarter)
        as_seen = ((owner[0] - to[0]) % chips, (owner[1] + to[1]) % CORES)
        dst_tile, dst_part = place(as_seen, quarter)
        idx = PEER_SLOT[as_seen] * 4 + quarter
        return pltpu.make_async_remote_copy(
            src_ref=h_all.at[src_tile, parts[src_part]], dst_ref=h_all.at[dst_tile, parts[dst_part]],
            send_sem=ag_send.at[idx], recv_sem=ag_recv.at[idx], device_id={"fsdp": dev(*to)}, device_id_type=MESH)

    def gather_recv(owner, quarter):
        dst_tile, dst_part = place(owner, quarter)
        idx = PEER_SLOT[owner] * 4 + quarter
        dst = h_all.at[dst_tile, parts[dst_part]]
        pltpu.make_async_remote_copy(
            src_ref=dst, dst_ref=dst, send_sem=ag_send.at[idx], recv_sem=ag_recv.at[idx],
            device_id={"fsdp": me}, device_id_type=MESH).wait_recv()

    for quarter in range(4):
        for to in (right, left, PARTNER):
            gather_copy(OWN, quarter, to).start()

    def target_copy(peer):
        slot = seen_from(peer)
        return pltpu.make_async_remote_copy(
            src_ref=t_all.at[me], dst_ref=t_all.at[me], send_sem=tgt_send.at[slot], recv_sem=tgt_recv.at[slot],
            device_id={"fsdp": dev(*peer)}, device_id_type=MESH)

    for peer in PEERS:
        target_copy(peer).start()
    load_w.wait()

    def pieces(tid):
        step, sub = lax.div(tid, 2), lax.rem(tid, 2)
        is_own = 1 - lax.div(lax.div(step, 2) + 3, 4)
        is_across = lax.div(step, 6)
        mixed = 1 - is_own - is_across
        flip = is_own * step + (1 - is_own) * sub
        j = is_own * sub + (1 - is_own) * (step - 2 - 4 * is_across)
        out = []
        for part in range(2):
            dx = mixed * (RIGHT, LEFT)[part] + is_across * ACROSS
            quarter = mixed * j + is_own * (2 * j + part) + is_across * (j + 2 * part)
            out.append((dev(dx, flip), quarter))
        return out

    def stat_copy(peer, block):
        return pltpu.make_async_remote_copy(
            src_ref=stat_loc.at[block], dst_ref=stat_in.at[seen_from(peer), block],
            send_sem=stat_send, recv_sem=stat_recv, device_id={"fsdp": dev(*peer)}, device_id_type=MESH)

    def fwd_tile(buf, tid):
        run_max = jnp.full((8, tile), -jnp.inf, F32)
        run_sum = jnp.zeros((8, tile), F32)
        for chunk, (start, size) in enumerate(row_chunks):
            sl = slice(start, start + size)
            z_ref[buf, sl, :] = lax.dot_general(
                w_ref[sl, :], h_all[tid], (((1,), (1,)), ((), ())), preferred_element_type=F32)
            for first, count in chunks(size, GROUP):
                z_grp = z_ref[buf, start + first:start + first + count, :].reshape(count // 8, 8, tile)
                new_max = jnp.maximum(run_max, jnp.max(z_grp, axis=0))
                run_sum = run_sum * jnp.exp(run_max - new_max) + jnp.sum(jnp.exp(z_grp - new_max[None]), axis=0)
                run_max = new_max
            z_store(buf, tid, chunk).start()
        tot_max = jnp.max(run_max, axis=0, keepdims=True)
        tot_sum = jnp.sum(run_sum * jnp.exp(run_max - tot_max), axis=0, keepdims=True)
        for part, (block, quarter) in enumerate(pieces(tid)):
            lanes = slice(part * quarter_toks, (part + 1) * quarter_toks)
            stat_loc[block, quarter, 0] = tot_max[:, lanes]
            stat_loc[block, quarter, 1] = tot_sum[:, lanes]

    def fwd_pair(step, carry):
        @pl.when(step == 1)
        def _():
            for quarter in range(4):
                gather_recv(PARTNER, quarter)

        for j in range(4):
            @pl.when(step == 2 + j)
            def _():
                gather_recv(left, j)
                gather_recv(right, j)
                if j < 2:
                    gather_copy(left, j, right).start()
                else:
                    gather_copy(right, j, left).start()
                gather_copy(left, j, PARTNER).start()
                gather_copy(right, j, PARTNER).start()

        for j in range(2):
            @pl.when(step == 6 + j)
            def _():
                if j == 0:
                    for owner in [OWN] + PEERS[:5]:
                        for peer in PEERS:
                            stat_copy(peer, dev(*owner)).start()
                for quarter in (j, j + 2):
                    gather_recv(across, quarter)
                    gather_copy(across, quarter, PARTNER).start()

        @pl.when(step > 0)
        def _():
            for chunk in range(len(row_chunks)):
                z_store(0, 0, chunk).wait()

        fwd_tile(0, 2 * step)
        for j in range(4):
            @pl.when(step == 2 + j)
            def _():
                gather_recv((LEFT, 1), j)
                gather_recv((RIGHT, 1), j)

        for j in range(2):
            @pl.when(step == 6 + j)
            def _():
                gather_recv((ACROSS, 1), j)
                gather_recv((ACROSS, 1), j + 2)

        for chunk in range(len(row_chunks)):
            z_store(1, 0, chunk).wait()
        fwd_tile(1, 2 * step + 1)
        return carry

    lax.fori_loop(0, groups, fwd_pair, 0)

    for owner in PEERS[5:]:
        for peer in PEERS:
            stat_copy(peer, dev(*owner)).start()

    def pair_tile(pair, flip):
        return lax.rem(lax.shift_right_logical(jnp.int32(PAIR_CODE), 4 * pair), 16) + flip * (1 + lax.div(pair, 6))

    for buf in range(2):
        for chunk in range(len(row_chunks)):
            z_store(buf, 0, chunk).wait()
        z_load(buf, tile_id("across", 1 - buf, 0)).start()
    for peer in PEERS:
        target_copy(peer).wait_recv()
    all_stats = pltpu.make_async_remote_copy(
        src_ref=stat_in, dst_ref=stat_in, send_sem=stat_send, recv_sem=stat_recv, device_id={"fsdp": me}, device_id_type=MESH)
    all_stats.wait_recv()

    def d2d_copy(slot):
        return pltpu.make_async_remote_copy(
            src_ref=pbuf.at[slot], dst_ref=d2d_in.at[slot], send_sem=d2d_send.at[slot], recv_sem=d2d_recv.at[slot],
            device_id={"fsdp": dev(*PARTNER)}, device_id_type=MESH)

    def ici_copy(pair, part):
        kind, j = PAIRS[pair]
        if kind == "across":
            dst, recv = ring_in.at[part, j], ring_recv.at[part * 2 + j]
        else:
            dst, recv = fin_in.at[part, j // 2, parts[j % 2]], fin_recv.at[part * 4 + j]
        return pltpu.make_async_remote_copy(
            src_ref=pbuf.at[2 + pair % SUMS, parts[part]], dst_ref=dst, send_sem=ici_send.at[(pair % SUMS) * 2 + part], recv_sem=recv,
            device_id={"fsdp": dev(*(right, left)[part])}, device_id_type=MESH)

    def wait_ici_sends(slot):
        for part in range(2):
            pltpu.make_async_remote_copy(
                src_ref=pbuf.at[2 + slot, parts[part]], dst_ref=ring_in.at[0, 0], send_sem=ici_send.at[slot * 2 + part],
                recv_sem=ring_recv.at[0], device_id={"fsdp": me}, device_id_type=MESH).wait_send()

    def add_into(slot, base, count, sources, dst=None):
        def body(i, carry):
            off = pl.multiple_of(i * 64, 64)
            sl = pl.ds(base + off, 64)
            tot = pbuf[slot, sl, :]
            for src in sources:
                tot = tot + src[pl.ds(off, 64), :]
            if dst is None:
                pbuf[slot, sl, :] = tot
            else:
                dst[sl, :] = tot
            return carry
        lax.fori_loop(0, count // 64, body, 0)

    inv_tokens = 1.0 / tokens
    log_tokens = jnp.log(jnp.float32(tokens))

    def bwd_tile(buf, tid, dh_slot=None, with_dw=True):
        where = pieces(tid)
        stats = [stat_loc] + [stat_in.at[i] for i in range(len(PEERS))]
        maxes, sums = [
            [jnp.concatenate([ref[block, quarter, kind] for block, quarter in where], axis=1) for ref in stats] for kind in range(2)]
        tot_max = functools.reduce(jnp.maximum, maxes)
        tot_sum = sum(s * jnp.exp(m - tot_max) for m, s in zip(maxes, sums))
        lse = tot_max + jnp.log(tot_sum)
        shift = lse + log_tokens
        tgt = jnp.concatenate([t_all[block, quarter] for block, quarter in where], axis=1) - me * rows
        if dh_slot is not None:
            lse_acc[...] += lse
            zt_sum = zt_acc[...]
        for idx, (start, size) in enumerate(row_chunks):
            sl = slice(start, start + size)
            z = z_ref[buf, sl, :]
            mask = (lax.broadcasted_iota(jnp.int32, (size, tile), 0) + start) == tgt
            prob = jnp.exp(z - shift)
            dz_ref[idx % 2, :size, :] = jnp.where(mask, prob - inv_tokens, prob).astype(BF16)
            if with_dw:
                dw_ref[sl, :] += jnp.dot(dz_ref[idx % 2, :size, :], h_all[tid], preferred_element_type=F32)
            if dh_slot is not None:
                zt_sum += jnp.sum(jnp.where(mask, z, 0.0).reshape(size // 8, 8, tile), axis=0)
                dh_part = lax.dot_general(dz_ref[idx % 2, :size, :], w_ref[sl, :], (((0,), (0,)), ((), ())), preferred_element_type=F32)
                if idx == 0:
                    pbuf[dh_slot] = dh_part
                else:
                    pbuf[dh_slot] += dh_part
        if dh_slot is not None:
            zt_acc[...] = zt_sum

    def finish_pair(pair):
        kind, j = PAIRS[pair]
        slot = 2 + pair % SUMS
        if kind == "own":
            for part in range(2):
                for q in range(2):
                    ici_copy(2 + 2 * j + q, part).wait_recv()
            add_into(slot, 0, tile, [d2d_in.at[pair % 2], fin_in.at[0, j], fin_in.at[1, j]], dh_ref.at[j])
            return
        for part in range(2):
            sources = [d2d_in.at[pair % 2, parts[part]]]
            if kind == "mixed" and j // 2 == part:
                ici_copy(j % 2, part).wait_recv()
                sources.append(ring_in.at[part, j % 2])
            add_into(slot, part * quarter_toks, quarter_toks, sources)
            ici_copy(pair, part).start()

    def run_pair(pair, odd, slot, with_dw):
        z_next = lax.rem(pair + 1, len(PAIRS))
        bwd_tile(0, pair_tile(pair, 1), odd, with_dw)
        d2d_copy(odd).start()
        z_load(0, pair_tile(z_next, 1)).start()
        z_load(1, 0).wait()
        bwd_tile(1, pair_tile(pair, 0), 2 + slot, with_dw)
        z_load(1, pair_tile(z_next, 0)).start()
        d2d_copy(odd).wait_recv()

    def bwd_pair(pair, carry):
        odd = lax.rem(pair, 2)

        @pl.when(pair >= 2)
        def _():
            d2d_copy(odd).wait_send()

        @pl.when(pair >= SUMS)
        def _():
            wait_ici_sends(lax.rem(pair, SUMS))

        z_load(0, 0).wait()
        run_pair(pair, odd, lax.rem(pair, SUMS), True)
        for pair_s in range(1, last):
            @pl.when(pair == pair_s)
            def _():
                finish_pair(pair_s)
        return carry

    last = len(PAIRS) - 1
    z_load(0, 0).wait()
    run_pair(jnp.int32(0), 0, 0, False)
    finish_pair(0)
    lax.fori_loop(1, last + 1, bwd_pair, 0)

    zt_row[...] = jnp.sum(zt_acc[...], axis=0, keepdims=True)

    def zt_copy(peer):
        slot = seen_from(peer)
        return pltpu.make_async_remote_copy(
            src_ref=zt_row, dst_ref=zt_in.at[slot], send_sem=zt_send.at[slot], recv_sem=zt_recv.at[slot],
            device_id={"fsdp": dev(*peer)}, device_id_type=MESH)

    for peer in PEERS:
        zt_copy(peer).start()
    for buf in range(2):
        z_load(buf, 0).wait()
        bwd_tile(buf, tile_id("across", 1 - buf, 0))
    finish_pair(last)
    for peer in PEERS:
        zt_copy(peer).wait()
    tot = lse_acc[...] - zt_row[...]
    for i in range(len(PEERS)):
        tot = tot - zt_in[i]
    loss_ref[...] = jnp.broadcast_to(jnp.sum(tot, axis=1, keepdims=True) * inv_tokens, loss_ref.shape)

    for owner, quarter, to in (
            [(OWN, q, to) for q in range(4) for to in (right, left, PARTNER)]
            + [(left, q, right) for q in (0, 1)] + [(right, q, left) for q in (2, 3)]
            + [(side, q, PARTNER) for side in (left, right, across) for q in range(4)]):
        gather_copy(owner, quarter, to).wait_send()
    for peer in PEERS:
        target_copy(peer).wait_send()
    all_stats.wait_send()
    for slot in range(2):
        d2d_copy(slot).wait_send()
    for pair in range(8 - SUMS, 6):
        wait_ici_sends(pair % SUMS)


def solution(mesh):
    groups = mesh.shape["fsdp"]
    tok_spec = P(("dp", "fsdp"), None)

    def local_head(hidden, targets, weight):
        tok_loc, width = hidden.shape
        rows = weight.shape[0]
        tokens = tok_loc * groups
        tile, quarter = tok_loc // 2, tok_loc // 4
        peers = len(PEERS)
        any_spec = pl.BlockSpec(memory_space=pl.ANY)
        vmem, dma = pltpu.VMEM, pltpu.SemaphoreType.DMA
        shape = jax.ShapeDtypeStruct
        loss_row, grad_h, grad_w, _ = pl.pallas_call(
            functools.partial(head_kernel, groups, tokens),
            in_specs=[any_spec] * 3,
            out_specs=[pl.BlockSpec(memory_space=pltpu.VMEM)] * 3 + [any_spec],
            out_shape=[
                shape((1, 128), F32), vmem((2, tile, width), F32), vmem((rows, width), F32), shape((2 * groups + 1, rows, tile), F32)],
            scratch_shapes=[
                vmem((2 * groups, tile, width), BF16),
                vmem((groups, 4, 1, quarter), jnp.int32),
                vmem((rows, width), BF16),
                vmem((2, rows, tile), F32),
                vmem((2, CHUNK, tile), BF16),
                vmem((2 + SUMS, tile, width), F32),
                vmem((2, tile, width), F32),
                vmem((2, 2, quarter, width), F32),
                vmem((2, 2, tile, width), F32),
                vmem((groups, 4, 2, 1, quarter), F32),
                vmem((peers, groups, 4, 2, 1, quarter), F32),
                vmem((1, tile), F32),
                vmem((8, tile), F32),
                vmem((1, tile), F32),
                vmem((peers, 1, tile), F32),
                dma((4,)), dma((4 * peers,)), dma((4 * peers,)), dma((peers,)), dma((peers,)), dma, dma,
                dma((2,)), dma((2,)), dma((2 * SUMS,)), dma((4,)), dma((8,)), dma((peers,)), dma((peers,)),
                dma((2, len(chunks(rows, CHUNK)))), dma((2,)),
            ],
            compiler_params=pltpu.CompilerParams(collective_id=0, has_side_effects=True, vmem_limit_bytes=VMEM_LIMIT),
            name="head",
        )(hidden.reshape(2, tile, width), targets.reshape(4, 1, quarter), weight)
        return loss_row[0, :1], grad_h.reshape(tok_loc, width), grad_w

    return jax.shard_map(local_head, mesh=mesh, in_specs=(tok_spec, P(("dp", "fsdp")), P("fsdp", None)), out_specs=(P("dp"), tok_spec, tok_spec), check_vma=False)
```

```python
import functools

import jax
import jax.numpy as jnp
from jax import lax
from jax.experimental import pallas as pl
from jax.experimental.pallas import tpu as pltpu
from jax.sharding import PartitionSpec as P

F32 = jnp.float32
BF16 = jnp.bfloat16
MESH = pl.DeviceIdType.MESH
CORES = 2
CHUNK = 1008
GROUP = 112
SUMS = 3
VMEM_LIMIT = 53_000_000

LEFT, RIGHT, ACROSS = 3, 1, 2
OWN, PARTNER = (0, 0), (0, 1)
PEERS = [PARTNER, (LEFT, 0), (LEFT, 1), (RIGHT, 0), (RIGHT, 1), (ACROSS, 0), (ACROSS, 1)]
PEER_SLOT = {peer: slot for slot, peer in enumerate(PEERS)}

def tile_id(kind, flip, j):
    if kind == "own":
        return 2 * flip + j
    return {"mixed": 4, "across": 12}[kind] + 2 * j + flip


def place(owner, quarter):
    dx, flip = owner
    if dx in (LEFT, RIGHT):
        return tile_id("mixed", flip, quarter), 0 if dx == RIGHT else 1
    if dx == ACROSS:
        return tile_id("across", flip, quarter % 2), quarter // 2
    return tile_id("own", flip, quarter // 2), quarter % 2


PAIRS = [("across", 0), ("across", 1)] + [("mixed", j) for j in range(4)] + [("own", 0), ("own", 1)]
PAIR_CODE = sum(tile_id(kind, 0, j) << (4 * q) for q, (kind, j) in enumerate(PAIRS))


def chunks(rows, step):
    return [(start, min(step, rows - start)) for start in range(0, rows, step)]


def head_kernel(groups, tokens, hid_hbm, tgt_hbm, w_hbm, loss_ref, pbuf, dw_ref, z_hbm,
                h_all, t_all, w_ref, z_ref, dz_ref, d2d_in, ring_in, fin_in,
                stat_loc, stat_in, lse_acc, zt_acc, zt_row, zt_in,
                load_sem, ag_send, ag_recv, tgt_send, tgt_recv, stat_send, stat_recv,
                d2d_send, d2d_recv, ici_send, ring_recv, fin_recv, zt_send, zt_recv, z_out, z_back):
    chips = groups // CORES
    me = lax.axis_index("fsdp")
    chip = lax.div(me, CORES)
    core = lax.rem(me, CORES)
    rows, width = w_ref.shape
    tile = h_all.shape[1]
    quarter_toks = tile // 2
    parts = [pl.ds(0, quarter_toks), pl.ds(quarter_toks, quarter_toks)]
    left, right, across = (LEFT, 0), (RIGHT, 0), (ACROSS, 0)

    def dev(dx, flip):
        return lax.rem(chip + dx, chips) * CORES + lax.rem(core + flip, CORES)

    def seen_from(peer):
        return PEER_SLOT[((chips - peer[0]) % chips, peer[1])]

    loads = [pltpu.make_async_copy(hid_hbm.at[j], h_all.at[tile_id("own", 0, j)], load_sem.at[j]) for j in range(2)]
    loads.append(pltpu.make_async_copy(tgt_hbm, t_all.at[me], load_sem.at[2]))
    load_w = pltpu.make_async_copy(w_hbm, w_ref, load_sem.at[3])
    for load in loads:
        load.start()
    load_w.start()
    barrier = pltpu.get_barrier_semaphore()
    for peer in PEERS:
        pl.semaphore_signal(barrier, inc=1, device_id={"fsdp": dev(*peer)}, device_id_type=MESH)
    dw_ref[...] = jnp.zeros_like(dw_ref)
    lse_acc[...] = jnp.zeros_like(lse_acc)
    zt_acc[...] = jnp.zeros_like(zt_acc)

    row_chunks = chunks(rows, CHUNK)

    def z_store(buf, slot, chunk):
        start, size = row_chunks[chunk]
        return pltpu.make_async_copy(z_ref.at[buf, start:start + size], z_hbm.at[slot, start:start + size], z_out.at[buf, chunk])

    def z_load(buf, slot):
        return pltpu.make_async_copy(z_hbm.at[slot], z_ref.at[buf], z_back.at[buf])

    for chunk, (start, size) in enumerate(row_chunks):
        pltpu.make_async_copy(dw_ref.at[start:start + size], z_hbm.at[2 * groups, start:start + size], z_out.at[1, chunk]).start()
    for load in loads:
        load.wait()
    pl.semaphore_wait(barrier, len(PEERS))

    def gather_copy(owner, quarter, to):
        src_tile, src_part = place(owner, quarter)
        as_seen = ((owner[0] - to[0]) % chips, (owner[1] + to[1]) % CORES)
        dst_tile, dst_part = place(as_seen, quarter)
        idx = PEER_SLOT[as_seen] * 4 + quarter
        return pltpu.make_async_remote_copy(
            src_ref=h_all.at[src_tile, parts[src_part]], dst_ref=h_all.at[dst_tile, parts[dst_part]],
            send_sem=ag_send.at[idx], recv_sem=ag_recv.at[idx], device_id={"fsdp": dev(*to)}, device_id_type=MESH)

    def gather_recv(owner, quarter):
        dst_tile, dst_part = place(owner, quarter)
        idx = PEER_SLOT[owner] * 4 + quarter
        dst = h_all.at[dst_tile, parts[dst_part]]
        pltpu.make_async_remote_copy(
            src_ref=dst, dst_ref=dst, send_sem=ag_send.at[idx], recv_sem=ag_recv.at[idx],
            device_id={"fsdp": me}, device_id_type=MESH).wait_recv()

    for quarter in range(4):
        for to in (right, left, PARTNER):
            gather_copy(OWN, quarter, to).start()

    def target_copy(peer):
        slot = seen_from(peer)
        return pltpu.make_async_remote_copy(
            src_ref=t_all.at[me], dst_ref=t_all.at[me], send_sem=tgt_send.at[slot], recv_sem=tgt_recv.at[slot],
            device_id={"fsdp": dev(*peer)}, device_id_type=MESH)

    for peer in PEERS:
        target_copy(peer).start()
    load_w.wait()

    def pieces(tid):
        step, sub = lax.div(tid, 2), lax.rem(tid, 2)
        is_own = 1 - lax.div(lax.div(step, 2) + 3, 4)
        is_across = lax.div(step, 6)
        mixed = 1 - is_own - is_across
        flip = is_own * step + (1 - is_own) * sub
        j = is_own * sub + (1 - is_own) * (step - 2 - 4 * is_across)
        out = []
        for part in range(2):
            dx = mixed * (RIGHT, LEFT)[part] + is_across * ACROSS
            quarter = mixed * j + is_own * (2 * j + part) + is_across * (j + 2 * part)
            out.append((dev(dx, flip), quarter))
        return out

    def stat_copy(peer, block):
        return pltpu.make_async_remote_copy(
            src_ref=stat_loc.at[block], dst_ref=stat_in.at[seen_from(peer), block],
            send_sem=stat_send, recv_sem=stat_recv, device_id={"fsdp": dev(*peer)}, device_id_type=MESH)

    def fwd_tile(buf, tid):
        run_max = jnp.full((8, tile), -jnp.inf, F32)
        run_sum = jnp.zeros((8, tile), F32)
        for chunk, (start, size) in enumerate(row_chunks):
            sl = slice(start, start + size)
            z_ref[buf, sl, :] = lax.dot_general(
                w_ref[sl, :], h_all[tid], (((1,), (1,)), ((), ())), preferred_element_type=F32)
            for first, count in chunks(size, GROUP):
                z_grp = z_ref[buf, start + first:start + first + count, :].reshape(count // 8, 8, tile)
                new_max = jnp.maximum(run_max, jnp.max(z_grp, axis=0))
                run_sum = run_sum * jnp.exp(run_max - new_max) + jnp.sum(jnp.exp(z_grp - new_max[None]), axis=0)
                run_max = new_max
            z_store(buf, tid, chunk).start()
        tot_max = jnp.max(run_max, axis=0, keepdims=True)
        tot_sum = jnp.sum(run_sum * jnp.exp(run_max - tot_max), axis=0, keepdims=True)
        for part, (block, quarter) in enumerate(pieces(tid)):
            lanes = slice(part * quarter_toks, (part + 1) * quarter_toks)
            stat_loc[block, quarter, 0] = tot_max[:, lanes]
            stat_loc[block, quarter, 1] = tot_sum[:, lanes]

    def fwd_pair(step, carry):
        @pl.when(step == 1)
        def _():
            for quarter in range(4):
                gather_recv(PARTNER, quarter)

        for j in range(4):
            @pl.when(step == 2 + j)
            def _():
                gather_recv(left, j)
                gather_recv(right, j)
                if j < 2:
                    gather_copy(left, j, right).start()
                else:
                    gather_copy(right, j, left).start()
                gather_copy(left, j, PARTNER).start()
                gather_copy(right, j, PARTNER).start()

        for j in range(2):
            @pl.when(step == 6 + j)
            def _():
                if j == 0:
                    for owner in [OWN] + PEERS[:5]:
                        for peer in PEERS:
                            stat_copy(peer, dev(*owner)).start()
                for quarter in (j, j + 2):
                    gather_recv(across, quarter)
                    gather_copy(across, quarter, PARTNER).start()

        @pl.when(step > 0)
        def _():
            for chunk in range(len(row_chunks)):
                z_store(0, 0, chunk).wait()

        fwd_tile(0, 2 * step)
        for j in range(4):
            @pl.when(step == 2 + j)
            def _():
                gather_recv((LEFT, 1), j)
                gather_recv((RIGHT, 1), j)

        for j in range(2):
            @pl.when(step == 6 + j)
            def _():
                gather_recv((ACROSS, 1), j)
                gather_recv((ACROSS, 1), j + 2)

        for chunk in range(len(row_chunks)):
            z_store(1, 0, chunk).wait()
        fwd_tile(1, 2 * step + 1)
        return carry

    lax.fori_loop(0, groups, fwd_pair, 0)

    for owner in PEERS[5:]:
        for peer in PEERS:
            stat_copy(peer, dev(*owner)).start()

    def pair_tile(pair, flip):
        return lax.rem(lax.shift_right_logical(jnp.int32(PAIR_CODE), 4 * pair), 16) + flip * (1 + lax.div(pair, 6))

    for buf in range(2):
        for chunk in range(len(row_chunks)):
            z_store(buf, 0, chunk).wait()
        z_load(buf, tile_id("across", 1 - buf, 0)).start()
    for peer in PEERS:
        target_copy(peer).wait_recv()
    all_stats = pltpu.make_async_remote_copy(
        src_ref=stat_in, dst_ref=stat_in, send_sem=stat_send, recv_sem=stat_recv, device_id={"fsdp": me}, device_id_type=MESH)
    all_stats.wait_recv()

    def d2d_copy(slot):
        return pltpu.make_async_remote_copy(
            src_ref=pbuf.at[slot], dst_ref=d2d_in.at[slot], send_sem=d2d_send.at[slot], recv_sem=d2d_recv.at[slot],
            device_id={"fsdp": dev(*PARTNER)}, device_id_type=MESH)

    def ici_copy(pair, part):
        kind, j = PAIRS[pair]
        if kind == "across":
            dst, recv = ring_in.at[part, j], ring_recv.at[part * 2 + j]
        else:
            dst, recv = fin_in.at[part, j // 2, parts[j % 2]], fin_recv.at[part * 4 + j]
        return pltpu.make_async_remote_copy(
            src_ref=pbuf.at[2 + pair % SUMS, parts[part]], dst_ref=dst, send_sem=ici_send.at[(pair % SUMS) * 2 + part], recv_sem=recv,
            device_id={"fsdp": dev(*(right, left)[part])}, device_id_type=MESH)

    def wait_ici_sends(slot):
        for part in range(2):
            pltpu.make_async_remote_copy(
                src_ref=pbuf.at[2 + slot, parts[part]], dst_ref=ring_in.at[0, 0], send_sem=ici_send.at[slot * 2 + part],
                recv_sem=ring_recv.at[0], device_id={"fsdp": me}, device_id_type=MESH).wait_send()

    def add_into(slot, base, count, sources):
        def body(i, carry):
            off = pl.multiple_of(i * 64, 64)
            sl = pl.ds(base + off, 64)
            tot = pbuf[slot, sl, :]
            for src in sources:
                tot = tot + src[pl.ds(off, 64), :]
            pbuf[slot, sl, :] = tot
            return carry
        lax.fori_loop(0, count // 64, body, 0)

    inv_tokens = 1.0 / tokens
    log_tokens = jnp.log(jnp.float32(tokens))

    def bwd_tile(buf, tid, dh_slot=None, with_dw=True):
        where = pieces(tid)
        stats = [stat_loc] + [stat_in.at[i] for i in range(len(PEERS))]
        maxes, sums = [
            [jnp.concatenate([ref[block, quarter, kind] for block, quarter in where], axis=1) for ref in stats] for kind in range(2)]
        tot_max = functools.reduce(jnp.maximum, maxes)
        tot_sum = sum(s * jnp.exp(m - tot_max) for m, s in zip(maxes, sums))
        lse = tot_max + jnp.log(tot_sum)
        shift = lse + log_tokens
        tgt = jnp.concatenate([t_all[block, quarter] for block, quarter in where], axis=1) - me * rows
        if dh_slot is not None:
            lse_acc[...] += lse
            zt_sum = zt_acc[...]
        for idx, (start, size) in enumerate(row_chunks):
            sl = slice(start, start + size)
            z = z_ref[buf, sl, :]
            mask = (lax.broadcasted_iota(jnp.int32, (size, tile), 0) + start) == tgt
            prob = jnp.exp(z - shift)
            dz_ref[sl, :] = jnp.where(mask, prob - inv_tokens, prob).astype(BF16)
            if with_dw:
                dw_ref[sl, :] += jnp.dot(dz_ref[sl, :], h_all[tid], preferred_element_type=F32)
            if dh_slot is not None:
                zt_sum += jnp.sum(jnp.where(mask, z, 0.0).reshape(size // 8, 8, tile), axis=0)
                dh_part = lax.dot_general(dz_ref[sl, :], w_ref[sl, :], (((0,), (0,)), ((), ())), preferred_element_type=F32)
                if idx == 0:
                    pbuf[dh_slot] = dh_part
                else:
                    pbuf[dh_slot] += dh_part
        if dh_slot is not None:
            zt_acc[...] = zt_sum

    def finish_pair(pair):
        kind, j = PAIRS[pair]
        slot = 2 + pair % SUMS
        if kind == "own":
            for part in range(2):
                for q in range(2):
                    ici_copy(2 + 2 * j + q, part).wait_recv()
            add_into(slot, 0, tile, [d2d_in.at[pair % 2], fin_in.at[0, j], fin_in.at[1, j]])
            return
        for part in range(2):
            sources = [d2d_in.at[pair % 2, parts[part]]]
            if kind == "mixed" and j // 2 == part:
                ici_copy(j % 2, part).wait_recv()
                sources.append(ring_in.at[part, j % 2])
            add_into(slot, part * quarter_toks, quarter_toks, sources)
            ici_copy(pair, part).start()

    def run_pair(pair, odd, slot, with_dw):
        z_next = lax.rem(pair + 1, len(PAIRS))
        bwd_tile(0, pair_tile(pair, 1), odd, with_dw)
        d2d_copy(odd).start()
        z_load(0, pair_tile(z_next, 1)).start()
        z_load(1, 0).wait()
        bwd_tile(1, pair_tile(pair, 0), 2 + slot, with_dw)
        z_load(1, pair_tile(z_next, 0)).start()
        d2d_copy(odd).wait_recv()

    def bwd_pair(pair, carry):
        odd = lax.rem(pair, 2)

        @pl.when(pair >= 2)
        def _():
            d2d_copy(odd).wait_send()

        @pl.when(pair >= SUMS)
        def _():
            wait_ici_sends(lax.rem(pair, SUMS))

        z_load(0, 0).wait()
        run_pair(pair, odd, lax.rem(pair, SUMS), True)
        for pair_s in range(1, last):
            @pl.when(pair == pair_s)
            def _():
                finish_pair(pair_s)
        return carry

    last = len(PAIRS) - 1
    z_load(0, 0).wait()
    run_pair(jnp.int32(0), 0, 0, False)
    finish_pair(0)
    lax.fori_loop(1, last + 1, bwd_pair, 0)

    zt_row[...] = jnp.sum(zt_acc[...], axis=0, keepdims=True)

    def zt_copy(peer):
        slot = seen_from(peer)
        return pltpu.make_async_remote_copy(
            src_ref=zt_row, dst_ref=zt_in.at[slot], send_sem=zt_send.at[slot], recv_sem=zt_recv.at[slot],
            device_id={"fsdp": dev(*peer)}, device_id_type=MESH)

    for peer in PEERS:
        zt_copy(peer).start()
    for buf in range(2):
        z_load(buf, 0).wait()
        bwd_tile(buf, tile_id("across", 1 - buf, 0))
    finish_pair(last)
    for peer in PEERS:
        zt_copy(peer).wait()
    tot = lse_acc[...] - zt_row[...]
    for i in range(len(PEERS)):
        tot = tot - zt_in[i]
    loss_ref[...] = jnp.broadcast_to(jnp.sum(tot, axis=1, keepdims=True) * inv_tokens, loss_ref.shape)

    for owner, quarter, to in (
            [(OWN, q, to) for q in range(4) for to in (right, left, PARTNER)]
            + [(left, q, right) for q in (0, 1)] + [(right, q, left) for q in (2, 3)]
            + [(side, q, PARTNER) for side in (left, right, across) for q in range(4)]):
        gather_copy(owner, quarter, to).wait_send()
    for peer in PEERS:
        target_copy(peer).wait_send()
    all_stats.wait_send()
    for slot in range(2):
        d2d_copy(slot).wait_send()
    for pair in range(8 - SUMS, 6):
        wait_ici_sends(pair % SUMS)


def solution(mesh):
    groups = mesh.shape["fsdp"]
    tok_spec = P(("dp", "fsdp"), None)

    def local_head(hidden, targets, weight):
        tok_loc, width = hidden.shape
        rows = weight.shape[0]
        tokens = tok_loc * groups
        tile, quarter = tok_loc // 2, tok_loc // 4
        peers = len(PEERS)
        any_spec = pl.BlockSpec(memory_space=pl.ANY)
        vmem, dma = pltpu.VMEM, pltpu.SemaphoreType.DMA
        shape = jax.ShapeDtypeStruct
        loss_row, sums, grad_w, _ = pl.pallas_call(
            functools.partial(head_kernel, groups, tokens),
            in_specs=[any_spec] * 3,
            out_specs=[pl.BlockSpec(memory_space=pltpu.VMEM)] * 3 + [any_spec],
            out_shape=[
                shape((1, 128), F32), vmem((2 + SUMS, tile, width), F32), vmem((rows, width), F32), shape((2 * groups + 1, rows, tile), F32)],
            scratch_shapes=[
                vmem((2 * groups, tile, width), BF16),
                vmem((groups, 4, 1, quarter), jnp.int32),
                vmem((rows, width), BF16),
                vmem((2, rows, tile), F32),
                vmem((rows, tile), BF16),
                vmem((2, tile, width), F32),
                vmem((2, 2, quarter, width), F32),
                vmem((2, 2, tile, width), F32),
                vmem((groups, 4, 2, 1, quarter), F32),
                vmem((peers, groups, 4, 2, 1, quarter), F32),
                vmem((1, tile), F32),
                vmem((8, tile), F32),
                vmem((1, tile), F32),
                vmem((peers, 1, tile), F32),
                dma((4,)), dma((4 * peers,)), dma((4 * peers,)), dma((peers,)), dma((peers,)), dma, dma,
                dma((2,)), dma((2,)), dma((2 * SUMS,)), dma((4,)), dma((8,)), dma((peers,)), dma((peers,)),
                dma((2, len(chunks(rows, CHUNK)))), dma((2,)),
            ],
            compiler_params=pltpu.CompilerParams(collective_id=0, has_side_effects=True, vmem_limit_bytes=VMEM_LIMIT),
            name="head",
        )(hidden.reshape(2, tile, width), targets.reshape(4, 1, quarter), weight)
        first = 2 + (len(PAIRS) - 2) % SUMS
        return loss_row[0, :1], sums[first:first + 2].reshape(tok_loc, width), grad_w

    return jax.shard_map(local_head, mesh=mesh, in_specs=(tok_spec, P(("dp", "fsdp")), P("fsdp", None)), out_specs=(P("dp"), tok_spec, tok_spec), check_vma=False)
```

```python
import functools

import jax
import jax.numpy as jnp
from jax import lax
from jax.experimental import pallas as pl
from jax.experimental.pallas import tpu as pltpu
from jax.sharding import PartitionSpec as P

F32 = jnp.float32
BF16 = jnp.bfloat16
MESH = pl.DeviceIdType.MESH
CORES = 2
CHUNK = 1008
GROUP = 112
SUMS = 3
VMEM_LIMIT = 53_000_000

LEFT, RIGHT, ACROSS = 3, 1, 2
OWN, PARTNER = (0, 0), (0, 1)
PEERS = [PARTNER, (LEFT, 0), (LEFT, 1), (RIGHT, 0), (RIGHT, 1), (ACROSS, 0), (ACROSS, 1)]
PEER_SLOT = {peer: slot for slot, peer in enumerate(PEERS)}

def tile_id(kind, flip, j):
    if kind == "own":
        return 2 * flip + j
    return {"mixed": 4, "across": 12}[kind] + 2 * j + flip


def place(owner, quarter):
    dx, flip = owner
    if dx in (LEFT, RIGHT):
        return tile_id("mixed", flip, quarter), 0 if dx == RIGHT else 1
    if dx == ACROSS:
        return tile_id("across", flip, quarter % 2), quarter // 2
    return tile_id("own", flip, quarter // 2), quarter % 2


PAIRS = [("across", 0), ("across", 1)] + [("mixed", j) for j in range(4)] + [("own", 0), ("own", 1)]
PAIR_CODE = sum(tile_id(kind, 0, j) << (4 * q) for q, (kind, j) in enumerate(PAIRS))


def chunks(rows, step):
    return [(start, min(step, rows - start)) for start in range(0, rows, step)]


def head_kernel(groups, tokens, hid_hbm, tgt_hbm, w_hbm, loss_ref, pbuf, dw_ref, z_hbm,
                h_all, t_all, w_ref, z_ref, dz_ref, d2d_in, ring_in, fin_in,
                stat_loc, stat_in, lse_acc, zt_acc, zt_row, zt_in,
                load_sem, ag_send, ag_recv, tgt_send, tgt_recv, stat_send, stat_recv,
                d2d_send, d2d_recv, ici_send, ring_recv, fin_recv, zt_send, zt_recv, z_out, z_back):
    chips = groups // CORES
    me = lax.axis_index("fsdp")
    chip = lax.div(me, CORES)
    core = lax.rem(me, CORES)
    rows, width = w_ref.shape
    tile = h_all.shape[1]
    quarter_toks = tile // 2
    parts = [pl.ds(0, quarter_toks), pl.ds(quarter_toks, quarter_toks)]
    left, right, across = (LEFT, 0), (RIGHT, 0), (ACROSS, 0)

    def dev(dx, flip):
        return lax.rem(chip + dx, chips) * CORES + lax.rem(core + flip, CORES)

    def seen_from(peer):
        return PEER_SLOT[((chips - peer[0]) % chips, peer[1])]

    loads = [pltpu.make_async_copy(hid_hbm.at[j], h_all.at[tile_id("own", 0, j)], load_sem.at[j]) for j in range(2)]
    loads.append(pltpu.make_async_copy(tgt_hbm, t_all.at[me], load_sem.at[2]))
    load_w = pltpu.make_async_copy(w_hbm, w_ref, load_sem.at[3])
    for load in loads:
        load.start()
    load_w.start()
    barrier = pltpu.get_barrier_semaphore()
    for peer in PEERS:
        pl.semaphore_signal(barrier, inc=1, device_id={"fsdp": dev(*peer)}, device_id_type=MESH)
    dw_ref[...] = jnp.zeros_like(dw_ref)
    lse_acc[...] = jnp.zeros_like(lse_acc)
    zt_acc[...] = jnp.zeros_like(zt_acc)

    row_chunks = chunks(rows, CHUNK)

    def z_store(buf, slot, chunk):
        start, size = row_chunks[chunk]
        return pltpu.make_async_copy(z_ref.at[buf, start:start + size], z_hbm.at[slot, start:start + size], z_out.at[buf, chunk])

    def z_load(buf, slot):
        return pltpu.make_async_copy(z_hbm.at[slot], z_ref.at[buf], z_back.at[buf])

    for chunk, (start, size) in enumerate(row_chunks):
        pltpu.make_async_copy(dw_ref.at[start:start + size], z_hbm.at[2 * groups, start:start + size], z_out.at[1, chunk]).start()
    for load in loads:
        load.wait()
    pl.semaphore_wait(barrier, len(PEERS))

    def gather_copy(owner, quarter, to):
        src_tile, src_part = place(owner, quarter)
        as_seen = ((owner[0] - to[0]) % chips, (owner[1] + to[1]) % CORES)
        dst_tile, dst_part = place(as_seen, quarter)
        idx = PEER_SLOT[as_seen] * 4 + quarter
        return pltpu.make_async_remote_copy(
            src_ref=h_all.at[src_tile, parts[src_part]], dst_ref=h_all.at[dst_tile, parts[dst_part]],
            send_sem=ag_send.at[idx], recv_sem=ag_recv.at[idx], device_id={"fsdp": dev(*to)}, device_id_type=MESH)

    def gather_recv(owner, quarter):
        dst_tile, dst_part = place(owner, quarter)
        idx = PEER_SLOT[owner] * 4 + quarter
        dst = h_all.at[dst_tile, parts[dst_part]]
        pltpu.make_async_remote_copy(
            src_ref=dst, dst_ref=dst, send_sem=ag_send.at[idx], recv_sem=ag_recv.at[idx],
            device_id={"fsdp": me}, device_id_type=MESH).wait_recv()

    for quarter in range(4):
        for to in (right, left, PARTNER):
            gather_copy(OWN, quarter, to).start()

    def target_copy(peer):
        slot = seen_from(peer)
        return pltpu.make_async_remote_copy(
            src_ref=t_all.at[me], dst_ref=t_all.at[me], send_sem=tgt_send.at[slot], recv_sem=tgt_recv.at[slot],
            device_id={"fsdp": dev(*peer)}, device_id_type=MESH)

    for peer in PEERS:
        target_copy(peer).start()
    load_w.wait()

    def pieces(tid):
        step, sub = lax.div(tid, 2), lax.rem(tid, 2)
        is_own = 1 - lax.div(lax.div(step, 2) + 3, 4)
        is_across = lax.div(step, 6)
        mixed = 1 - is_own - is_across
        flip = is_own * step + (1 - is_own) * sub
        j = is_own * sub + (1 - is_own) * (step - 2 - 4 * is_across)
        out = []
        for part in range(2):
            dx = mixed * (RIGHT, LEFT)[part] + is_across * ACROSS
            quarter = mixed * j + is_own * (2 * j + part) + is_across * (j + 2 * part)
            out.append((dev(dx, flip), quarter))
        return out

    def stat_copy(peer, block):
        return pltpu.make_async_remote_copy(
            src_ref=stat_loc.at[block], dst_ref=stat_in.at[seen_from(peer), block],
            send_sem=stat_send, recv_sem=stat_recv, device_id={"fsdp": dev(*peer)}, device_id_type=MESH)

    def fwd_tile(buf, tid):
        run_max = jnp.full((8, tile), -jnp.inf, F32)
        run_sum = jnp.zeros((8, tile), F32)
        for chunk, (start, size) in enumerate(row_chunks):
            sl = slice(start, start + size)
            z_ref[buf, sl, :] = lax.dot_general(
                w_ref[sl, :], h_all[tid], (((1,), (1,)), ((), ())), preferred_element_type=F32)
            for first, count in chunks(size, GROUP):
                z_grp = z_ref[buf, start + first:start + first + count, :].reshape(count // 8, 8, tile)
                new_max = jnp.maximum(run_max, jnp.max(z_grp, axis=0))
                run_sum = run_sum * jnp.exp(run_max - new_max) + jnp.sum(jnp.exp(z_grp - new_max[None]), axis=0)
                run_max = new_max
            z_store(buf, tid, chunk).start()
        tot_max = jnp.max(run_max, axis=0, keepdims=True)
        tot_sum = jnp.sum(run_sum * jnp.exp(run_max - tot_max), axis=0, keepdims=True)
        for part, (block, quarter) in enumerate(pieces(tid)):
            lanes = slice(part * quarter_toks, (part + 1) * quarter_toks)
            stat_loc[block, quarter, 0] = tot_max[:, lanes]
            stat_loc[block, quarter, 1] = tot_sum[:, lanes]

    def fwd_pair(step, carry):
        @pl.when(step == 1)
        def _():
            for quarter in range(4):
                gather_recv(PARTNER, quarter)

        for j in range(4):
            @pl.when(step == 2 + j)
            def _():
                gather_recv(left, j)
                gather_recv(right, j)
                if j < 2:
                    gather_copy(left, j, right).start()
                else:
                    gather_copy(right, j, left).start()
                gather_copy(left, j, PARTNER).start()
                gather_copy(right, j, PARTNER).start()

        for j in range(2):
            @pl.when(step == 6 + j)
            def _():
                if j == 0:
                    for owner in [OWN] + PEERS[:5]:
                        for peer in PEERS:
                            stat_copy(peer, dev(*owner)).start()
                for quarter in (j, j + 2):
                    gather_recv(across, quarter)
                    gather_copy(across, quarter, PARTNER).start()

        @pl.when(step > 0)
        def _():
            for chunk in range(len(row_chunks)):
                z_store(0, 0, chunk).wait()

        fwd_tile(0, 2 * step)
        for j in range(4):
            @pl.when(step == 2 + j)
            def _():
                gather_recv((LEFT, 1), j)
                gather_recv((RIGHT, 1), j)

        for j in range(2):
            @pl.when(step == 6 + j)
            def _():
                gather_recv((ACROSS, 1), j)
                gather_recv((ACROSS, 1), j + 2)

        for chunk in range(len(row_chunks)):
            z_store(1, 0, chunk).wait()
        fwd_tile(1, 2 * step + 1)
        return carry

    lax.fori_loop(0, groups, fwd_pair, 0)

    for owner in PEERS[5:]:
        for peer in PEERS:
            stat_copy(peer, dev(*owner)).start()

    def pair_tile(pair, flip):
        return lax.rem(lax.shift_right_logical(jnp.int32(PAIR_CODE), 4 * pair), 16) + flip * (1 + lax.div(pair, 6))

    for buf in range(2):
        for chunk in range(len(row_chunks)):
            z_store(buf, 0, chunk).wait()
        z_load(buf, tile_id("across", 1 - buf, 0)).start()
    for peer in PEERS:
        target_copy(peer).wait_recv()
    all_stats = pltpu.make_async_remote_copy(
        src_ref=stat_in, dst_ref=stat_in, send_sem=stat_send, recv_sem=stat_recv, device_id={"fsdp": me}, device_id_type=MESH)
    all_stats.wait_recv()

    def d2d_copy(slot):
        return pltpu.make_async_remote_copy(
            src_ref=pbuf.at[slot], dst_ref=d2d_in.at[slot], send_sem=d2d_send.at[slot], recv_sem=d2d_recv.at[slot],
            device_id={"fsdp": dev(*PARTNER)}, device_id_type=MESH)

    def ici_copy(pair, part):
        kind, j = PAIRS[pair]
        if kind == "across":
            dst, recv = ring_in.at[part, j], ring_recv.at[part * 2 + j]
        else:
            dst, recv = fin_in.at[part, j // 2, parts[j % 2]], fin_recv.at[part * 4 + j]
        return pltpu.make_async_remote_copy(
            src_ref=pbuf.at[2 + pair % SUMS, parts[part]], dst_ref=dst, send_sem=ici_send.at[(pair % SUMS) * 2 + part], recv_sem=recv,
            device_id={"fsdp": dev(*(right, left)[part])}, device_id_type=MESH)

    def wait_ici_sends(slot):
        for part in range(2):
            pltpu.make_async_remote_copy(
                src_ref=pbuf.at[2 + slot, parts[part]], dst_ref=ring_in.at[0, 0], send_sem=ici_send.at[slot * 2 + part],
                recv_sem=ring_recv.at[0], device_id={"fsdp": me}, device_id_type=MESH).wait_send()

    def add_into(slot, base, count, sources):
        def body(i, carry):
            off = pl.multiple_of(i * 64, 64)
            sl = pl.ds(base + off, 64)
            tot = pbuf[slot, sl, :]
            for src in sources:
                tot = tot + src[pl.ds(off, 64), :]
            pbuf[slot, sl, :] = tot
            return carry
        lax.fori_loop(0, count // 64, body, 0)

    inv_tokens = 1.0 / tokens
    log_tokens = jnp.log(jnp.float32(tokens))

    def bwd_tile(buf, tid, dh_slot=None, with_dw=True):
        where = pieces(tid)
        stats = [stat_loc] + [stat_in.at[i] for i in range(len(PEERS))]
        maxes, sums = [
            [jnp.concatenate([ref[block, quarter, kind] for block, quarter in where], axis=1) for ref in stats] for kind in range(2)]
        tot_max = functools.reduce(jnp.maximum, maxes)
        tot_sum = sum(s * jnp.exp(m - tot_max) for m, s in zip(maxes, sums))
        lse = tot_max + jnp.log(tot_sum)
        shift = lse + log_tokens
        tgt = jnp.concatenate([t_all[block, quarter] for block, quarter in where], axis=1) - me * rows
        if dh_slot is not None:
            lse_acc[...] += lse
            zt_sum = zt_acc[...]
        for idx, (start, size) in enumerate(row_chunks):
            sl = slice(start, start + size)
            z = z_ref[buf, sl, :]
            mask = (lax.broadcasted_iota(jnp.int32, (size, tile), 0) + start) == tgt
            prob = jnp.exp(z - shift)
            dz_ref[sl, :] = jnp.where(mask, prob - inv_tokens, prob).astype(BF16)
            if with_dw:
                dw_ref[sl, :] += jnp.dot(dz_ref[sl, :], h_all[tid], preferred_element_type=F32)
            if dh_slot is not None:
                zt_sum += jnp.sum(jnp.where(mask, z, 0.0).reshape(size // 8, 8, tile), axis=0)
                dh_part = lax.dot_general(dz_ref[sl, :], w_ref[sl, :], (((0,), (0,)), ((), ())), preferred_element_type=F32)
                if idx == 0:
                    pbuf[dh_slot] = dh_part
                else:
                    pbuf[dh_slot] += dh_part
        if dh_slot is not None:
            zt_acc[...] = zt_sum

    def finish_pair(pair):
        kind, j = PAIRS[pair]
        slot = 2 + pair % SUMS
        if kind == "own":
            for part in range(2):
                for q in range(2):
                    ici_copy(2 + 2 * j + q, part).wait_recv()
            add_into(slot, 0, tile, [d2d_in.at[pair % 2], fin_in.at[0, j], fin_in.at[1, j]])
            return
        for part in range(2):
            sources = [d2d_in.at[pair % 2, parts[part]]]
            if kind == "mixed" and j // 2 == part:
                ici_copy(j % 2, part).wait_recv()
                sources.append(ring_in.at[part, j % 2])
            add_into(slot, part * quarter_toks, quarter_toks, sources)
            ici_copy(pair, part).start()

    def run_pair(pair, odd, slot, with_dw):
        z_next = lax.rem(pair + 1, len(PAIRS))
        bwd_tile(0, pair_tile(pair, 1), odd, with_dw)
        d2d_copy(odd).start()
        z_load(0, pair_tile(z_next, 1)).start()
        z_load(1, 0).wait()
        bwd_tile(1, pair_tile(pair, 0), 2 + slot, with_dw)

        @pl.when(pair < last)
        def _():
            z_load(1, pair_tile(z_next, 0)).start()

        d2d_copy(odd).wait_recv()

    def bwd_pair(pair, carry):
        odd = lax.rem(pair, 2)

        @pl.when(pair >= 2)
        def _():
            d2d_copy(odd).wait_send()

        @pl.when(pair >= SUMS)
        def _():
            wait_ici_sends(lax.rem(pair, SUMS))

        z_load(0, 0).wait()
        run_pair(pair, odd, lax.rem(pair, SUMS), True)
        for pair_s in range(1, last):
            @pl.when(pair == pair_s)
            def _():
                finish_pair(pair_s)
        return carry

    last = len(PAIRS) - 1
    z_load(0, 0).wait()
    run_pair(jnp.int32(0), 0, 0, True)
    finish_pair(0)
    lax.fori_loop(1, last + 1, bwd_pair, 0)

    zt_row[...] = jnp.sum(zt_acc[...], axis=0, keepdims=True)

    def zt_copy(peer):
        slot = seen_from(peer)
        return pltpu.make_async_remote_copy(
            src_ref=zt_row, dst_ref=zt_in.at[slot], send_sem=zt_send.at[slot], recv_sem=zt_recv.at[slot],
            device_id={"fsdp": dev(*peer)}, device_id_type=MESH)

    for peer in PEERS:
        zt_copy(peer).start()
    z_load(0, 0).wait()
    finish_pair(last)
    for peer in PEERS:
        zt_copy(peer).wait()
    tot = lse_acc[...] - zt_row[...]
    for i in range(len(PEERS)):
        tot = tot - zt_in[i]
    loss_ref[...] = jnp.broadcast_to(jnp.sum(tot, axis=1, keepdims=True) * inv_tokens, loss_ref.shape)

    for owner, quarter, to in (
            [(OWN, q, to) for q in range(4) for to in (right, left, PARTNER)]
            + [(left, q, right) for q in (0, 1)] + [(right, q, left) for q in (2, 3)]
            + [(side, q, PARTNER) for side in (left, right, across) for q in range(4)]):
        gather_copy(owner, quarter, to).wait_send()
    for peer in PEERS:
        target_copy(peer).wait_send()
    all_stats.wait_send()
    for slot in range(2):
        d2d_copy(slot).wait_send()
    for pair in range(8 - SUMS, 6):
        wait_ici_sends(pair % SUMS)


def solution(mesh):
    groups = mesh.shape["fsdp"]
    tok_spec = P(("dp", "fsdp"), None)

    def local_head(hidden, targets, weight):
        tok_loc, width = hidden.shape
        rows = weight.shape[0]
        tokens = tok_loc * groups
        tile, quarter = tok_loc // 2, tok_loc // 4
        peers = len(PEERS)
        any_spec = pl.BlockSpec(memory_space=pl.ANY)
        vmem, dma = pltpu.VMEM, pltpu.SemaphoreType.DMA
        shape = jax.ShapeDtypeStruct
        loss_row, sums, grad_w, _ = pl.pallas_call(
            functools.partial(head_kernel, groups, tokens),
            in_specs=[any_spec] * 3,
            out_specs=[pl.BlockSpec(memory_space=pltpu.VMEM)] * 3 + [any_spec],
            out_shape=[
                shape((1, 128), F32), vmem((2 + SUMS, tile, width), F32), vmem((rows, width), F32), shape((2 * groups + 1, rows, tile), F32)],
            scratch_shapes=[
                vmem((2 * groups, tile, width), BF16),
                vmem((groups, 4, 1, quarter), jnp.int32),
                vmem((rows, width), BF16),
                vmem((2, rows, tile), F32),
                vmem((rows, tile), BF16),
                vmem((2, tile, width), F32),
                vmem((2, 2, quarter, width), F32),
                vmem((2, 2, tile, width), F32),
                vmem((groups, 4, 2, 1, quarter), F32),
                vmem((peers, groups, 4, 2, 1, quarter), F32),
                vmem((1, tile), F32),
                vmem((8, tile), F32),
                vmem((1, tile), F32),
                vmem((peers, 1, tile), F32),
                dma((4,)), dma((4 * peers,)), dma((4 * peers,)), dma((peers,)), dma((peers,)), dma, dma,
                dma((2,)), dma((2,)), dma((2 * SUMS,)), dma((4,)), dma((8,)), dma((peers,)), dma((peers,)),
                dma((2, len(chunks(rows, CHUNK)))), dma((2,)),
            ],
            compiler_params=pltpu.CompilerParams(collective_id=0, has_side_effects=True, vmem_limit_bytes=VMEM_LIMIT),
            name="head",
        )(hidden.reshape(2, tile, width), targets.reshape(4, 1, quarter), weight)
        first = 2 + (len(PAIRS) - 2) % SUMS
        return loss_row[0, :1], sums[first:first + 2].reshape(tok_loc, width), grad_w

    return jax.shard_map(local_head, mesh=mesh, in_specs=(tok_spec, P(("dp", "fsdp")), P("fsdp", None)), out_specs=(P("dp"), tok_spec, tok_spec), check_vma=False)
```
